128 devices in a mesh: row: 16 (over z, y), col: 8 (over x, core).
Axes of the slice: x: 4, y: 4, z: 4, core: 2. Of those that a mesh axis runs over, the one named last changes fastest.
Arguments:
- params: float32 [4, 4096, 10240], P(None, ('row', 'col'))
- grads: bfloat16 [4, 4096, 10240], P(None, ('row', 'col')), may hold values from -6 to 6
- row_state_old: float32 [4, 4096], P(None, ('row', 'col')), may hold values from 0.05 to 0.5
- col_state_old: float32 [4, 10240], P(None, ('row', 'col')), may hold values from 0.05 to 0.5
- old_map: int32 [4, 128], replicated, may hold values from 0 to 127, each once within a row
- new_map: int32 [4, 128], replicated, may hold values from 0 to 127, each once within a row
Outputs:
- new_params: float32 [4, 4096, 10240], P(None, 'row', 'col')
- step_change: float32 [4, 4096, 10240], P(None, 'row', 'col')
- row_state: float32 [4, 4096], P(None, ('row', 'col'))
- col_state: float32 [4, 10240], P(None, ('row', 'col'))
The draws below stay inside these ranges and needn't reach their ends.
Inputs may be any that keep to these rules, and one draw needn't show every extreme that they name: Each row of old_map is a permutation of 0 to 127. Each row of new_map is a permutation of 0 to 127.
All inputs are finite; a program needn't handle non-finite values.
Results may differ from the reference program's by a relative error of at most 0.0003.
Values may be sent and summed in bfloat16 or wider, within the bound.
A program may use at most 128 MiB of HBM per device.

```python
import math
import jax
import jax.numpy as jnp
from jax import lax

D = 4096
FF = 10240
STEP = 4
NMAT = 4
BLOCKS = 128


def draw_params(key, part):
    first_key = jax.random.fold_in(jax.random.fold_in(key, 11), 0)
    rising = 0.5 * 3.0 ** (jnp.arange(D, dtype=jnp.float32) / D)
    values = jax.random.normal(first_key, (NMAT, D, FF), jnp.float32)
    return (values * rising[None, :, None]).astype(jnp.float32)


def steps_of(key, shape, cuts, least, top_value):
    gain, own = 1.0, jax.random.fold_in(key, 6)
    for dim, parts in cuts:
        steps = jnp.exp(jax.random.uniform(jax.random.fold_in(own, dim), (parts,), jnp.float32, least / len(cuts), top_value / len(cuts)))
        gain = gain * jnp.repeat(steps, shape[dim] // parts).reshape([-1 if axis == dim else 1 for axis in range(len(shape))])
    return gain


def scatter_about(stream_key, shape, deviation, limit, shards=(), kind=jnp.bfloat16):
    drawn = deviation * jax.random.normal(stream_key, shape, jnp.float32)
    if shards:
        drawn = drawn * steps_of(stream_key, shape, shards, -0.22, 0.18)
    return jnp.clip(drawn, -limit, limit).astype(kind)


def setup_inputs(seed: int = 0) -> dict:
    arg_keys = jax.random.split(jax.random.key(seed), 7)
    return {
        "params": draw_params(jax.random.fold_in(arg_keys[6], 71), 0),
        "grads": scatter_about(arg_keys[1], (NMAT, D, FF), 1.0, 6.0, ((1, 128),)),
        "row_state_old": jnp.clip(jnp.exp(math.log(0.5) - 2.3025851 * jax.random.uniform(arg_keys[2], (NMAT, D), jnp.float32) ** steps_of(arg_keys[2], (NMAT, D), ((1, 128),), -0.2, 0.2)), 0.05, 0.5),
        "col_state_old": jnp.clip(jnp.exp(math.log(0.5) - 2.3025851 * jax.random.uniform(arg_keys[3], (NMAT, FF), jnp.float32) ** steps_of(arg_keys[3], (NMAT, FF), ((1, 128),), -0.2, 0.2)), 0.05, 0.5),
        "old_map": jax.vmap(lambda own: jax.random.permutation(own, BLOCKS))(jax.random.split(arg_keys[4], NMAT)).reshape((NMAT, BLOCKS)).astype(jnp.int32),
        "new_map": jax.vmap(lambda own: jax.random.permutation(own, BLOCKS))(jax.random.split(arg_keys[5], NMAT)).reshape((NMAT, BLOCKS)).astype(jnp.int32),
    }


eps_square = 1e-30
clip_limit = 1.0

def unpermute(stored, order):
    matrices = stored.shape[0]
    pieces = stored.reshape(matrices, order.shape[1], -1)
    inverse = jnp.argsort(order, axis=1).astype(jnp.int32)
    return jnp.take_along_axis(pieces, inverse[:, :, None], axis=1).reshape(matrices, -1)

def permute(logical, order):
    matrices = logical.shape[0]
    pieces = logical.reshape(matrices, order.shape[1], -1)
    return jnp.take_along_axis(pieces, order[:, :, None], axis=1).reshape(matrices, -1)

def reference(params, grads, row_state_old, col_state_old, old_map, new_map):
    decay_rate = 1.0 - float(STEP) ** (-0.8)
    step_rate = min(0.01, 1.0 / math.sqrt(STEP))
    row_old = unpermute(row_state_old, old_map)
    col_old = unpermute(col_state_old, old_map)
    gradient = grads.astype(jnp.float32)
    squares = gradient * gradient + eps_square
    row_new = decay_rate * row_old + (1.0 - decay_rate) * lax.optimization_barrier(jnp.sum(squares, axis=2)) / FF
    col_new = decay_rate * col_old + (1.0 - decay_rate) * lax.optimization_barrier(jnp.sum(squares, axis=1)) / D
    row_mean = lax.optimization_barrier(jnp.mean(row_new, axis=1))
    variance = row_new[:, :, None] * col_new[:, None, :] / row_mean[:, None, None]
    update = gradient / jnp.sqrt(variance)
    clip_factor = jnp.maximum(1.0, jnp.sqrt(jnp.mean(update * update)) / clip_limit)
    param_scale = jnp.sqrt(lax.optimization_barrier(jnp.mean(params * params, axis=(1, 2))) + 1e-06)
    step_change = -(step_rate * param_scale)[:, None, None] * update / clip_factor
    new_params = params + step_change
    return (new_params, step_change, permute(row_new, new_map), permute(col_new, new_map))
```

```python
import functools
import math

import jax
import jax.numpy as jnp
from jax import lax
from jax.experimental import pallas as pl
from jax.experimental.pallas import tpu as pltpu
from jax.sharding import Mesh
from jax.sharding import PartitionSpec as P

D = 4096
FF = 10240
STEP = 4
M = 4
ROWS = 32
COLS = 1280
AXES = ("z", "y", "x", "c")
MESH = pl.DeviceIdType.MESH
HIGHEST = lax.Precision.HIGHEST
DECAY = 1.0 - float(STEP) ** (-0.8)
RATE = min(0.01, 1.0 / math.sqrt(STEP))
EPS = 1e-30
F32 = jnp.float32
FIRST = 1

COL_PEERS = [(1, 0), (3, 0), (2, 0), (1, 1), (3, 1), (2, 1), (0, 1)]
LINE_PEERS = [1, 2, 3]


def iota(shape, dim):
    return lax.broadcasted_iota(jnp.int32, shape, dim)


def exchange_kernel(
    params, grads, row_old, col_old, old_map,
    p_out, g_out, r_out, c_out, rows_out, cols_out,
    gv, pv, stored, row_tiles, red_y, red_z, sc_x, sc_y, sc_z, sel, rnew,
    load_sem, own_sem,
    s_tile, r_tile, s_line, r_line, s_grad, r_grad, s_par, r_par,
    s_row, r_row, s_red, r_red, s_sc, r_sc, s_col, r_col,
):
    z, y, x, c = (lax.axis_index(a) for a in AXES)
    k = x * 2 + c
    f = (z * 4 + y) * 8 + k

    def col_peer(i):
        dx, dc = COL_PEERS[i]
        return lax.rem(x + dx, 4), lax.rem(c + dc, 2)

    def to_cols(i, src, dst, ss, rs):
        tx, tc = col_peer(i)
        return pltpu.make_async_remote_copy(
            src_ref=src, dst_ref=dst, send_sem=ss, recv_sem=rs,
            device_id={"x": tx, "c": tc}, device_id_type=MESH,
        )

    def to_line(axis, d, src, dst, ss, rs):
        at = lax.rem((y if axis == "y" else z) + d, 4)
        return pltpu.make_async_remote_copy(
            src_ref=src, dst_ref=dst, send_sem=ss, recv_sem=rs,
            device_id={axis: at}, device_id_type=MESH,
        )

    def begin(copies):
        for cp in copies:
            cp.start()
        return copies

    def arrive(copies):
        for cp in copies:
            cp.wait_recv()

    loads = []
    for m in range(M):
        loads.append(pltpu.make_async_copy(grads.at[m], gv.at[m], load_sem.at[m]))
    for m in range(M):
        loads.append(pltpu.make_async_copy(params.at[m], pv.at[m], load_sem.at[M + m]))
    begin(loads)

    barrier = pltpu.get_barrier_semaphore()
    for i in range(7):
        tx, tc = col_peer(i)
        pl.semaphore_signal(barrier, inc=1, device_id={"x": tx, "c": tc}, device_id_type=MESH)
    for d in LINE_PEERS:
        pl.semaphore_signal(barrier, inc=1, device_id={"y": lax.rem(y + d, 4)}, device_id_type=MESH)
        pl.semaphore_signal(barrier, inc=1, device_id={"z": lax.rem(z + d, 4)}, device_id_type=MESH)

    mine = stored.at[pl.ds(pl.multiple_of(f * 8, 8), 8)]
    mine[...] = jnp.zeros((8, 128), F32)
    mine[0:4, 0:80] = col_old[...]
    mine[4:8, 0:32] = row_old[...]

    pl.semaphore_wait(barrier, 13)

    tiles = begin([to_cols(i, mine, mine, s_tile.at[i], r_tile.at[i]) for i in range(7)])
    sent = list(tiles)

    def columns(i):
        tx, tc = col_peer(i)
        return pl.ds(pl.multiple_of((tx * 2 + tc) * COLS, 128), COLS)

    grad_copies = begin(
        [to_cols(i, grads.at[:, :, columns(i)], g_out.at[k], s_grad.at[i], r_grad.at[i]) for i in range(7)]
    )
    sent += grad_copies

    def send_params(m):
        copies = begin(
            [
                to_cols(i, params.at[m, :, columns(i)], p_out.at[k, m], s_par.at[m, i], r_par.at[m, i])
                for i in range(7)
            ]
        )
        sent.extend(copies)
        return copies

    par_copies = []
    for m in range(FIRST):
        par_copies += send_params(m)

    own_columns = pl.ds(pl.multiple_of(k * COLS, 128), COLS)
    lane32 = iota((ROWS, 128), 1)
    row_sums = jnp.zeros((ROWS, 128), F32)
    own = []
    for m in range(M):
        loads[m].wait()

        def add_squares(t, acc, m=m):
            g = gv[m, :, pl.ds(pl.multiple_of(t * COLS, 128), COLS)].astype(F32)
            sq = g * g + EPS
            for u in range(COLS // 128):
                acc = acc + sq[:, u * 128 : (u + 1) * 128]
            return acc

        part = lax.fori_loop(0, 8, add_squares, jnp.zeros((ROWS, 128), F32))
        total = jnp.sum(part, axis=1, keepdims=True)
        row_sums = row_sums + jnp.where(lane32 == m, total, 0.0)
        own.append(pltpu.make_async_copy(gv.at[m, :, own_columns], g_out.at[k, m], own_sem.at[m]))
        own[-1].start()

    arrive(tiles)
    line_at = stored.at[pl.ds(pl.multiple_of((z * 4 + y) * 64, 64), 64)]
    lines = begin([to_line("y", d, line_at, line_at, s_line.at[d - 1], r_line.at[d - 1]) for d in LINE_PEERS])
    sent += lines

    lane8 = iota((8, 128), 1)
    squares = jnp.zeros((8, 128), F32)
    for m in range(M):
        loads[M + m].wait()

        def add_weights(t, acc, m=m):
            w = pv[m, :, pl.ds(pl.multiple_of(t * COLS, 128), COLS)]
            sq = w * w
            for u in range(COLS // 128):
                for v in range(ROWS // 8):
                    acc = acc + sq[v * 8 : (v + 1) * 8, u * 128 : (u + 1) * 128]
            return acc

        part = lax.fori_loop(0, 8, add_weights, jnp.zeros((8, 128), F32))
        total = jnp.sum(jnp.sum(part, axis=1, keepdims=True), axis=0, keepdims=True)
        squares = squares + jnp.where(lane8 == m, total, 0.0)
        own.append(pltpu.make_async_copy(pv.at[m, :, own_columns], p_out.at[k, m], own_sem.at[M + m]))
        own[-1].start()

    arrive(lines)
    slab_at = stored.at[pl.ds(pl.multiple_of(z * 256, 256), 256)]
    slabs = begin([to_line("z", d, slab_at, slab_at, s_line.at[d + 2], r_line.at[d + 2]) for d in LINE_PEERS])
    sent += slabs
    arrive(slabs)

    at_row = iota((128, 128), 0)
    picked = jnp.zeros((128, 128), F32)
    for m in range(M):
        onehot = jnp.where((at_row == m) & (old_map[m : m + 1, :] == f), 1.0, 0.0)
        picked = picked + jnp.dot(
            onehot, stored[pl.ds(4 + m, 128, stride=8), :], precision=HIGHEST, preferred_element_type=F32
        )
    row_block = jnp.transpose(picked)[0:ROWS, :]
    row_new = DECAY * row_block + (1.0 - DECAY) * row_sums / FF
    row_tiles[k, 0:ROWS, :] = jnp.where(lane32 < M, row_new, 1.0)
    row_tiles[k, ROWS : ROWS + 8, :] = jnp.where(iota((8, 128), 0) == 0, squares, 0.0)
    row_copies = begin(
        [to_cols(i, row_tiles.at[k], row_tiles.at[k], s_row.at[i], r_row.at[i]) for i in range(7)]
    )
    sent += row_copies

    lane = iota((1, COLS), 1)
    block_of = ((lane.astype(F32) + 0.5) * (1.0 / 80.0)).astype(jnp.int32)
    place_of = lane - 80 * block_of
    at64 = iota((64, 128), 0)
    blocks = jnp.zeros((64, 128), F32)
    for m in range(M):
        wanted = (at64 - 16 * m) + k * 16
        inside = (at64 >= 16 * m) & (at64 < 16 * m + 16)
        onehot = jnp.where(inside & (old_map[m : m + 1, :] == wanted), 1.0, 0.0)
        blocks = blocks + jnp.dot(
            onehot, stored[pl.ds(m, 128, stride=8), :], precision=HIGHEST, preferred_element_type=F32
        )
    sel[0:64, 0:128] = blocks
    spread = jnp.where(iota((128, COLS), 0) == place_of, 1.0, 0.0)
    wide = jnp.dot(sel[0:64, 0:128], spread, precision=HIGHEST, preferred_element_type=F32)
    sel[...] = wide
    at16 = iota((16, COLS), 0)
    old_cols = [
        jnp.sum(jnp.where(at16 == block_of, sel[m * 16 : (m + 1) * 16, :], 0.0), axis=0, keepdims=True)
        for m in range(M)
    ]
    for m in range(M):
        c_out[m : m + 1, :] = old_cols[m]

    arrive(grad_copies)
    for m in range(M):
        own[m].wait()

    red_y[y, 4:8, :] = jnp.zeros((4, COLS), F32)
    for m in range(M):

        def add_columns(t, acc, m=m):
            g = g_out[t, m].astype(F32)
            sq = g * g + EPS
            for v in range(ROWS // 8):
                acc = acc + sq[v * 8 : (v + 1) * 8, :]
            return acc

        part = lax.fori_loop(0, 8, add_columns, jnp.zeros((8, COLS), F32))
        red_y[y, m : m + 1, :] = jnp.sum(part, axis=0, keepdims=True)

    arrive(row_copies)
    row_sum = jnp.zeros((1, 128), F32)
    weight_sum = jnp.zeros((1, 128), F32)
    for t in range(8):
        part = row_tiles[t, 0:ROWS, :]
        rnew[t * ROWS : (t + 1) * ROWS, :] = part
        row_sum = row_sum + jnp.sum(part, axis=0, keepdims=True)
        weight_sum = weight_sum + row_tiles[t, ROWS : ROWS + 1, :]
    red_y[y, 4:5, 0:128] = row_sum
    red_y[y, 5:6, 0:128] = weight_sum
    across = jnp.transpose(rnew[0:128, :]), jnp.transpose(rnew[128:256, :])
    own_row = z * 4 + y
    rows_out[own_row, :, 0:128] = across[0][0:8, :]
    rows_out[own_row, :, 128:256] = across[1][0:8, :]

    stage = begin(
        [to_line("y", d, red_y.at[y], red_y.at[y], s_red.at[d - 1], r_red.at[d - 1]) for d in LINE_PEERS]
    )
    own_rows = rows_out.at[pl.ds(own_row, 1)]
    rows_y = begin(
        [to_line("y", d, own_rows, own_rows, s_red.at[d + 5], r_red.at[d + 5]) for d in LINE_PEERS]
    )
    arrive(stage)
    sent += stage + rows_y
    red_z[z] = red_y[0] + red_y[1] + red_y[2] + red_y[3]
    stage = begin(
        [to_line("z", d, red_z.at[z], red_z.at[z], s_red.at[d + 2], r_red.at[d + 2]) for d in LINE_PEERS]
    )
    arrive(rows_y)
    slab_rows = rows_out.at[pl.ds(pl.multiple_of(z * 4, 4), 4)]
    rows_z = begin(
        [to_line("z", d, slab_rows, slab_rows, s_red.at[d + 8], r_red.at[d + 8]) for d in LINE_PEERS]
    )
    arrive(stage)
    sent += stage + rows_z
    total = red_z[0] + red_z[1] + red_z[2] + red_z[3]

    row_mean = total[4:5, 0:128] / D
    param_scale = jnp.sqrt(total[5:6, 0:128] / (D * FF) + 1e-6)
    col_new = DECAY * c_out[0:M, :] + (1.0 - DECAY) * total[0:M, :] / D
    cols_out[k] = col_new
    sel[0:M, :] = 1.0 / col_new

    update_sum = jnp.zeros((8, 128), F32)
    for m in range(M):
        inv_col = sel[m : m + 1, :]

        def add_updates(t, acc, m=m, inv_col=inv_col):
            g = g_out[t, m].astype(F32)
            sq = g * g * inv_col
            part = sq[:, 0:128]
            for u in range(1, COLS // 128):
                part = part + sq[:, u * 128 : (u + 1) * 128]
            rows = rnew[pl.ds(pl.multiple_of(t * ROWS, ROWS), ROWS), :][:, m : m + 1]
            part = part / rows
            for v in range(ROWS // 8):
                acc = acc + part[v * 8 : (v + 1) * 8, :]
            return acc

        part = lax.fori_loop(0, 8, add_updates, jnp.zeros((8, 128), F32))
        update_sum = update_sum + part * row_mean[0:1, m : m + 1]
    sc_x[k] = update_sum
    sums = begin([to_cols(i, sc_x.at[k], sc_x.at[k], s_sc.at[i], r_sc.at[i]) for i in range(7)])
    col_copies = begin(
        [to_cols(i, cols_out.at[k], cols_out.at[k], s_col.at[i], r_col.at[i]) for i in range(7)]
    )
    sent += sums + col_copies

    for m in range(FIRST, M):
        par_copies += send_params(m)

    arrive(sums)
    update_sum = sc_x[0]
    for t in range(1, 8):
        update_sum = update_sum + sc_x[t]
    sc_y[y] = update_sum
    stage = begin(
        [to_line("y", d, sc_y.at[y], sc_y.at[y], s_sc.at[d + 6], r_sc.at[d + 6]) for d in LINE_PEERS]
    )
    arrive(stage)
    sent += stage
    sc_z[z] = sc_y[0] + sc_y[1] + sc_y[2] + sc_y[3]
    stage = begin(
        [to_line("z", d, sc_z.at[z], sc_z.at[z], s_sc.at[d + 9], r_sc.at[d + 9]) for d in LINE_PEERS]
    )
    arrive(stage)
    sent += stage
    update_sum = sc_z[0] + sc_z[1] + sc_z[2] + sc_z[3]
    update_total = jnp.sum(jnp.sum(update_sum, axis=1, keepdims=True), axis=0, keepdims=True)
    clip = jnp.maximum(1.0, jnp.sqrt(update_total / (M * D * FF)))
    factor = -(RATE * param_scale) / clip * jnp.sqrt(row_mean)
    r_out[...] = factor / jnp.sqrt(rnew[...])
    c_out[0:M, :] = jnp.sqrt(sel[0:M, :])

    arrive(rows_z)
    arrive(col_copies)
    for m in range(M):
        own[M + m].wait()
    arrive(par_copies)
    for cp in sent:
        cp.wait_send()


def apply_kernel(quarter, q_ref, g_ref, r_ref, c_ref, rows_ref, cols_ref, map_ref, new_ref, change_ref, row_ref, col_ref):
    i = pl.program_id(0)
    m = i // quarter
    at = lax.rem(i, quarter)
    slots = 8 // quarter

    @pl.when(i == 0)
    def _():
        f = lax.axis_index(AXES)
        for n in range(M):
            b = map_ref[n, f]
            row = rows_ref[b // 8, n : n + 1, :]
            start = lax.rem(b, 8) * 32
            take = jnp.where(iota((256, 128), 0) == start + iota((256, 128), 1), 1.0, 0.0)
            got = jnp.dot(jnp.broadcast_to(row, (8, 256)), take, precision=HIGHEST, preferred_element_type=F32)
            row_ref[n : n + 1, :] = got[0:1, 0:32]
            col = cols_ref[b // 16, n : n + 1, :]
            start = lax.rem(b, 16) * 80
            take = jnp.where(iota((COLS, 128), 0) == start + iota((COLS, 128), 1), 1.0, 0.0)
            got = jnp.dot(jnp.broadcast_to(col, (8, COLS)), take, precision=HIGHEST, preferred_element_type=F32)
            col_ref[n : n + 1, :] = got[0:1, 0:80]

    lane = iota((ROWS, 128), 1)
    by_col = c_ref[pl.ds(m, 1), :]
    for s in range(slots):
        t = at * slots + s
        by_row = r_ref[pl.ds(pl.multiple_of(t * ROWS, ROWS), ROWS), :]
        by_row = jnp.sum(jnp.where(lane == m, by_row, 0.0), axis=1, keepdims=True)
        g = g_ref[t, m].astype(F32)
        change = (g * by_row) * by_col
        change_ref[0, s * ROWS : (s + 1) * ROWS, :] = change
        new_ref[0, s * ROWS : (s + 1) * ROWS, :] = q_ref[t, m] + change


def shards(params, grads, row_state_old, col_state_old, old_map, new_map):
    vmem = pl.BlockSpec(memory_space=pltpu.VMEM)
    hbm = pl.BlockSpec(memory_space=pl.ANY)
    dma = pltpu.SemaphoreType.DMA
    moved = pl.pallas_call(
        exchange_kernel,
        out_shape=[
            jax.ShapeDtypeStruct((8, M, ROWS, COLS), F32),
            jax.ShapeDtypeStruct((8, M, ROWS, COLS), jnp.bfloat16),
            jax.ShapeDtypeStruct((256, 128), F32),
            jax.ShapeDtypeStruct((8, COLS), F32),
            jax.ShapeDtypeStruct((16, 8, 256), F32),
            jax.ShapeDtypeStruct((8, M, COLS), F32),
        ],
        in_specs=[hbm, hbm, vmem, vmem, vmem],
        out_specs=[vmem] * 6,
        scratch_shapes=[
            pltpu.VMEM((M, ROWS, FF), jnp.bfloat16),
            pltpu.VMEM((M, ROWS, FF), F32),
            pltpu.VMEM((1024, 128), F32),
            pltpu.VMEM((8, ROWS + 8, 128), F32),
            pltpu.VMEM((4, 8, COLS), F32),
            pltpu.VMEM((4, 8, COLS), F32),
            pltpu.VMEM((8, 8, 128), F32),
            pltpu.VMEM((4, 8, 128), F32),
            pltpu.VMEM((4, 8, 128), F32),
            pltpu.VMEM((64, COLS), F32),
            pltpu.VMEM((256, 128), F32),
            dma((2 * M,)),
            dma((2 * M,)),
            dma((7,)), dma((7,)),
            dma((6,)), dma((6,)),
            dma((7,)), dma((7,)),
            dma((M, 7)), dma((M, 7)),
            dma((7,)), dma((7,)),
            dma((12,)), dma((12,)),
            dma((13,)), dma((13,)),
            dma((7,)), dma((7,)),
        ],
        compiler_params=pltpu.CompilerParams(
            collective_id=0, has_side_effects=True, vmem_limit_bytes=56 << 20
        ),
        name="exchange",
    )(params, grads, row_state_old, col_state_old, old_map)
    quarter = 4
    rows = 256 // quarter
    whole = pl.BlockSpec((1, rows, COLS), lambda i: (i // quarter, lax.rem(i, quarter), 0))
    return pl.pallas_call(
        functools.partial(apply_kernel, quarter),
        grid=(M * quarter,),
        out_shape=[
            jax.ShapeDtypeStruct((M, 256, COLS), F32),
            jax.ShapeDtypeStruct((M, 256, COLS), F32),
            jax.ShapeDtypeStruct((M, 32), F32),
            jax.ShapeDtypeStruct((M, 80), F32),
        ],
        in_specs=[vmem] * 6 + [pl.BlockSpec(memory_space=pltpu.SMEM)],
        out_specs=[
            whole,
            whole,
            pl.BlockSpec((M, 32), lambda i: (0, 0)),
            pl.BlockSpec((M, 80), lambda i: (0, 0)),
        ],
        compiler_params=pltpu.CompilerParams(vmem_limit_bytes=56 << 20),
        name="apply",
    )(*moved, new_map)


def solution(mesh):
    torus = Mesh(mesh.devices.reshape(4, 4, 4, 2), AXES)
    over = ("z", "y", "x", "c")
    return jax.shard_map(
        shards,
        mesh=torus,
        in_specs=(P(None, over, None), P(None, over, None), P(None, over), P(None, over), P(), P()),
        out_specs=(
            P(None, ("z", "y"), ("x", "c")),
            P(None, ("z", "y"), ("x", "c")),
            P(None, over),
            P(None, over),
        ),
        check_vma=False,
    )
```

```python
import functools
import math

import jax
import jax.numpy as jnp
from jax import lax
from jax.experimental import pallas as pl
from jax.experimental.pallas import tpu as pltpu
from jax.sharding import Mesh
from jax.sharding import PartitionSpec as P

D = 4096
FF = 10240
STEP = 4
M = 4
ROWS = 32
COLS = 1280
AXES = ("z", "y", "x", "c")
MESH = pl.DeviceIdType.MESH
HIGHEST = lax.Precision.HIGHEST
DECAY = 1.0 - float(STEP) ** (-0.8)
RATE = min(0.01, 1.0 / math.sqrt(STEP))
EPS = 1e-30
F32 = jnp.float32
TOP = 32767.0
CODED = False
FIRST = 2

COL_PEERS = [(1, 0), (3, 0), (2, 0), (1, 1), (3, 1), (2, 1), (0, 1)]
LINE_PEERS = [1, 2, 3]


def iota(shape, dim):
    return lax.broadcasted_iota(jnp.int32, shape, dim)


def exchange_kernel(
    params, grads, row_hbm, col_hbm, map_hbm,
    p_out, s_out, g_out, r_out, c_out, rows_out, cols_out,
    gv, pv, qv, sv, row_old, col_old, old_map, stored, row_tiles, red_y, red_z, sc_y, sc_z, sel, rnew,
    load_sem, small_sem, own_sem,
    s_tile, r_tile, s_line, r_line, s_grad, r_grad, s_par, r_par,
    s_row, r_row, s_red, r_red, s_sc, r_sc,
):
    z, y, x, c = (lax.axis_index(a) for a in AXES)
    k = x * 2 + c
    f = (z * 4 + y) * 8 + k

    def col_peer(i):
        dx, dc = COL_PEERS[i]
        return lax.rem(x + dx, 4), lax.rem(c + dc, 2)

    def to_cols(i, src, dst, ss, rs):
        tx, tc = col_peer(i)
        return pltpu.make_async_remote_copy(
            src_ref=src, dst_ref=dst, send_sem=ss, recv_sem=rs,
            device_id={"x": tx, "c": tc}, device_id_type=MESH,
        )

    def to_line(axis, d, src, dst, ss, rs):
        at = lax.rem((y if axis == "y" else z) + d, 4)
        return pltpu.make_async_remote_copy(
            src_ref=src, dst_ref=dst, send_sem=ss, recv_sem=rs,
            device_id={axis: at}, device_id_type=MESH,
        )

    def begin(copies):
        for cp in copies:
            cp.start()
        return copies

    def arrive(copies):
        for cp in copies:
            cp.wait_recv()

    small = [
        pltpu.make_async_copy(row_hbm, row_old, small_sem.at[0]),
        pltpu.make_async_copy(col_hbm, col_old, small_sem.at[1]),
        pltpu.make_async_copy(map_hbm, old_map, small_sem.at[2]),
    ]
    begin(small)
    loads = []
    for m in range(M):
        loads.append(pltpu.make_async_copy(grads.at[m], gv.at[m], load_sem.at[m]))
    for m in range(M):
        loads.append(pltpu.make_async_copy(params.at[m], pv.at[m], load_sem.at[M + m]))
    begin(loads)

    barrier = pltpu.get_barrier_semaphore()
    for i in range(7):
        tx, tc = col_peer(i)
        pl.semaphore_signal(barrier, inc=1, device_id={"x": tx, "c": tc}, device_id_type=MESH)
    for d in LINE_PEERS:
        pl.semaphore_signal(barrier, inc=1, device_id={"y": lax.rem(y + d, 4)}, device_id_type=MESH)
        pl.semaphore_signal(barrier, inc=1, device_id={"z": lax.rem(z + d, 4)}, device_id_type=MESH)

    mine = stored.at[pl.ds(pl.multiple_of(f * 8, 8), 8)]
    mine[...] = jnp.zeros((8, 128), F32)
    for cp in small:
        cp.wait()
    mine[0:4, 0:80] = col_old[...]
    mine[4:8, 0:32] = row_old[...]

    pl.semaphore_wait(barrier, 13)

    tiles = begin([to_cols(i, mine, mine, s_tile.at[i], r_tile.at[i]) for i in range(7)])
    sent = list(tiles)

    def columns(i):
        tx, tc = col_peer(i)
        return pl.ds(pl.multiple_of((tx * 2 + tc) * COLS, 128), COLS)

    grad_copies = begin(
        [to_cols(i, grads.at[:, :, columns(i)], g_out.at[k], s_grad.at[i], r_grad.at[i]) for i in range(7)]
    )
    sent += grad_copies

    def peer_block(i):
        tx, tc = col_peer(i)
        return tx * 2 + tc

    def send_params(m):
        if CODED:
            copies = [
                to_cols(i, qv.at[peer_block(i), m], p_out.at[k, m], s_par.at[m, i], r_par.at[m, i])
                for i in range(7)
            ]
        else:
            copies = [
                to_cols(i, params.at[m, :, columns(i)], p_out.at[k, m], s_par.at[m, i], r_par.at[m, i])
                for i in range(7)
            ]
        begin(copies)
        sent.extend(copies)
        return copies

    par_copies = []
    if not CODED:
        for m in range(FIRST):
            par_copies += send_params(m)

    own_columns = pl.ds(pl.multiple_of(k * COLS, 128), COLS)
    lane32 = iota((ROWS, 128), 1)
    row_sums = jnp.zeros((ROWS, 128), F32)
    own = []
    for m in range(M):
        loads[m].wait()

        def add_squares(t, acc, m=m):
            g = gv[m, :, pl.ds(pl.multiple_of(t * COLS, 128), COLS)].astype(F32)
            sq = g * g + EPS
            for u in range(COLS // 128):
                acc = acc + sq[:, u * 128 : (u + 1) * 128]
            return acc

        part = lax.fori_loop(0, 8, add_squares, jnp.zeros((ROWS, 128), F32))
        total = jnp.sum(part, axis=1, keepdims=True)
        row_sums = row_sums + jnp.where(lane32 == m, total, 0.0)
        own.append(pltpu.make_async_copy(gv.at[m, :, own_columns], g_out.at[k, m], own_sem.at[m]))
        own[-1].start()

    at8 = iota((8, 128), 0)
    lane8 = iota((8, 128), 1)
    squares = jnp.zeros((8, 128), F32)
    for m in range(M):
        loads[M + m].wait()

        def add_weights(t, acc, m=m):
            w = pv[m, :, pl.ds(pl.multiple_of(t * COLS, 128), COLS)]
            sq = w * w
            tops = [jnp.zeros((8, 128), F32)] * 2
            size = jnp.abs(w)
            for u in range(COLS // 128):
                for v in range(ROWS // 8):
                    acc = acc + sq[v * 8 : (v + 1) * 8, u * 128 : (u + 1) * 128]
                    if CODED:
                        tops[u % 2] = jnp.maximum(tops[u % 2], size[v * 8 : (v + 1) * 8, u * 128 : (u + 1) * 128])
            if CODED:
                top = jnp.concatenate([jnp.max(a, axis=0, keepdims=True) for a in tops], axis=1)
                top = jnp.maximum(top, 1e-30)
                sv[t, m : m + 1, :] = top * (1.0 / TOP)
                per = jnp.concatenate([TOP / top] * (COLS // 256), axis=1)
                qv[t, m] = jnp.round(w * per).astype(jnp.int32).astype(jnp.int16)
            return acc

        part = lax.fori_loop(0, 8, add_weights, jnp.zeros((8, 128), F32))
        total = jnp.sum(jnp.sum(part, axis=1, keepdims=True), axis=0, keepdims=True)
        squares = squares + jnp.where((at8 == m) & (lane8 == ROWS), total, 0.0)
        here = qv.at[k, m] if CODED else pv.at[m, :, own_columns]
        own.append(pltpu.make_async_copy(here, p_out.at[k, m], own_sem.at[M + m]))
        own[-1].start()
    if CODED:
        own.append(pltpu.make_async_copy(sv.at[k], s_out.at[k], own_sem.at[2 * M]))
        own[-1].start()
        par_copies += begin(
            [to_cols(i, sv.at[peer_block(i)], s_out.at[k], s_par.at[M, i], r_par.at[M, i]) for i in range(7)]
        )
        sent.extend(par_copies)
        for m in range(FIRST):
            par_copies += send_params(m)

    arrive(tiles)
    line_at = stored.at[pl.ds(pl.multiple_of((z * 4 + y) * 64, 64), 64)]
    lines = begin([to_line("y", d, line_at, line_at, s_line.at[d - 1], r_line.at[d - 1]) for d in LINE_PEERS])
    sent += lines

    arrive(lines)
    slab_at = stored.at[pl.ds(pl.multiple_of(z * 256, 256), 256)]
    slabs = begin([to_line("z", d, slab_at, slab_at, s_line.at[d + 2], r_line.at[d + 2]) for d in LINE_PEERS])
    sent += slabs
    arrive(slabs)

    at_row = iota((128, 128), 0)
    picked = jnp.zeros((128, 128), F32)
    for m in range(M):
        onehot = jnp.where((at_row == m) & (old_map[m : m + 1, :] == f), 1.0, 0.0)
        picked = picked + jnp.dot(
            onehot, stored[pl.ds(4 + m, 128, stride=8), :], precision=HIGHEST, preferred_element_type=F32
        )
    sel[...] = jnp.zeros((128, COLS), F32)
    sel[0:ROWS, 0:128] = row_sums
    row_sums = jnp.transpose(sel[:, 0:128])[0:8, :]
    row_new = DECAY * picked[0:8, :] + (1.0 - DECAY) * row_sums / FF
    row_new = jnp.where((at8 < M) & (lane8 < ROWS), row_new, 1.0)
    row_tiles[64:128, :] = jnp.ones((64, 128), F32)
    own_tile = row_tiles.at[pl.ds(pl.multiple_of(k * 8, 8), 8)]
    own_tile[...] = jnp.where(lane8 == ROWS, squares, row_new)
    row_copies = begin([to_cols(i, own_tile, own_tile, s_row.at[i], r_row.at[i]) for i in range(7)])
    sent += row_copies

    lane = iota((1, COLS), 1)
    block_of = ((lane.astype(F32) + 0.5) * (1.0 / 80.0)).astype(jnp.int32)
    place_of = lane - 80 * block_of
    at64 = iota((64, 128), 0)
    blocks = jnp.zeros((64, 128), F32)
    for m in range(M):
        wanted = (at64 - 16 * m) + k * 16
        inside = (at64 >= 16 * m) & (at64 < 16 * m + 16)
        onehot = jnp.where(inside & (old_map[m : m + 1, :] == wanted), 1.0, 0.0)
        blocks = blocks + jnp.dot(
            onehot, stored[pl.ds(m, 128, stride=8), :], precision=HIGHEST, preferred_element_type=F32
        )
    sel[0:64, 0:128] = blocks
    spread = jnp.where(iota((128, COLS), 0) == place_of, 1.0, 0.0)
    wide = jnp.dot(sel[0:64, 0:128], spread, precision=HIGHEST, preferred_element_type=F32)
    sel[0:64, :] = wide
    at16 = iota((16, COLS), 0)
    old_cols = [
        jnp.sum(jnp.where(at16 == block_of, sel[m * 16 : (m + 1) * 16, :], 0.0), axis=0, keepdims=True)
        for m in range(M)
    ]
    for m in range(M):
        c_out[m : m + 1, :] = old_cols[m]

    arrive(grad_copies)
    for m in range(M):
        own[m].wait()

    red_y[y, 4:8, :] = jnp.zeros((4, COLS), F32)
    for m in range(M):

        def add_columns(t, acc, m=m):
            g = g_out[t, m].astype(F32)
            sq = g * g + EPS
            for v in range(ROWS // 8):
                acc = acc + sq[v * 8 : (v + 1) * 8, :]
            return acc

        part = lax.fori_loop(0, 8, add_columns, jnp.zeros((8, COLS), F32))
        red_y[y, m : m + 1, :] = jnp.sum(part, axis=0, keepdims=True)

    arrive(row_copies)
    tile_sum = row_tiles[0:8, :]
    for t in range(1, 8):
        tile_sum = tile_sum + row_tiles[t * 8 : (t + 1) * 8, :]
    row_sum = jnp.sum(jnp.where(lane8 < ROWS, tile_sum, 0.0), axis=1, keepdims=True)
    weight_sum = jnp.sum(jnp.where(lane8 == ROWS, tile_sum, 0.0), axis=1, keepdims=True)
    both = jnp.where(lane8 == 0, row_sum, jnp.where(lane8 == 1, weight_sum, 0.0))
    red_y[y, 4:8, 0:128] = both[0:4, :]
    own_row = z * 4 + y
    rows_out[own_row] = row_tiles[0:64, :]

    stage = begin(
        [to_line("y", d, red_y.at[y], red_y.at[y], s_red.at[d - 1], r_red.at[d - 1]) for d in LINE_PEERS]
    )
    own_rows = rows_out.at[pl.ds(own_row, 1)]
    rows_y = begin(
        [to_line("y", d, own_rows, own_rows, s_red.at[d + 5], r_red.at[d + 5]) for d in LINE_PEERS]
    )
    arrive(stage)
    sent += stage + rows_y
    red_z[z] = red_y[0] + red_y[1] + red_y[2] + red_y[3]
    stage = begin(
        [to_line("z", d, red_z.at[z], red_z.at[z], s_red.at[d + 2], r_red.at[d + 2]) for d in LINE_PEERS]
    )
    arrive(rows_y)
    slab_rows = rows_out.at[pl.ds(pl.multiple_of(z * 4, 4), 4)]
    rows_z = begin(
        [to_line("z", d, slab_rows, slab_rows, s_red.at[d + 8], r_red.at[d + 8]) for d in LINE_PEERS]
    )
    arrive(stage)
    sent += stage + rows_z
    total = red_z[0] + red_z[1] + red_z[2] + red_z[3]

    row_mean = [total[4 + m : 5 + m, 0:1] / D for m in range(M)]
    param_scale = [jnp.sqrt(total[4 + m : 5 + m, 1:2] / (D * FF) + 1e-6) for m in range(M)]
    col_new = DECAY * c_out[0:M, :] + (1.0 - DECAY) * total[0:M, :] / D
    sel[0:M, :] = col_new
    piece = lax.min(own_row, COLS // 128 - 1)
    cols_out[own_row, k, 0:M, :] = sel[0:M, pl.ds(pl.multiple_of(piece * 128, 128), 128)]
    sel[0:M, :] = 1.0 / col_new
    new_rows = jnp.transpose(row_tiles[...])[0:ROWS, :]
    rnew[...] = 1.0 / new_rows

    update_sum = jnp.zeros((8, 128), F32)
    for m in range(M):
        inv_col = sel[m : m + 1, :]

        def add_updates(t, acc, m=m, inv_col=inv_col):
            g = g_out[t, m].astype(F32)
            sq = g * g * inv_col
            part = sq[:, 0:128]
            for u in range(1, COLS // 128):
                part = part + sq[:, u * 128 : (u + 1) * 128]
            part = part * jnp.sum(jnp.where(lane32 == t * 8 + m, rnew[...], 0.0), axis=1, keepdims=True)
            for v in range(ROWS // 8):
                acc = acc + part[v * 8 : (v + 1) * 8, :]
            return acc

        part = lax.fori_loop(0, 8, add_updates, jnp.zeros((8, 128), F32))
        update_sum = update_sum + part * row_mean[m]
    cols_out[own_row, k, 4:8, :] = update_sum[0:4, :] + update_sum[4:8, :]
    own_col = cols_out.at[own_row, k]
    sums = begin([to_cols(i, own_col, own_col, s_sc.at[i], r_sc.at[i]) for i in range(7)])
    sent += sums

    for m in range(FIRST, M):
        par_copies += send_params(m)

    arrive(sums)
    update_sum = cols_out[own_row, 0, 4:8, :]
    for t in range(1, 8):
        update_sum = update_sum + cols_out[own_row, t, 4:8, :]
    sc_y[y] = jnp.zeros((8, 128), F32)
    sc_y[y, 0:4, :] = update_sum
    stage = begin(
        [to_line("y", d, sc_y.at[y], sc_y.at[y], s_sc.at[d + 6], r_sc.at[d + 6]) for d in LINE_PEERS]
    )
    own_cols = cols_out.at[pl.ds(own_row, 1)]
    cols_y = begin(
        [to_line("y", d, own_cols, own_cols, s_sc.at[d + 12], r_sc.at[d + 12]) for d in LINE_PEERS]
    )
    arrive(stage)
    sent += stage + cols_y
    sc_z[z] = sc_y[0] + sc_y[1] + sc_y[2] + sc_y[3]
    stage = begin(
        [to_line("z", d, sc_z.at[z], sc_z.at[z], s_sc.at[d + 9], r_sc.at[d + 9]) for d in LINE_PEERS]
    )
    arrive(cols_y)
    slab_cols = cols_out.at[pl.ds(pl.multiple_of(z * 4, 4), 4)]
    cols_z = begin(
        [to_line("z", d, slab_cols, slab_cols, s_sc.at[d + 15], r_sc.at[d + 15]) for d in LINE_PEERS]
    )
    arrive(stage)
    sent += stage + cols_z
    update_sum = sc_z[0] + sc_z[1] + sc_z[2] + sc_z[3]
    update_total = jnp.sum(jnp.sum(update_sum, axis=1, keepdims=True), axis=0, keepdims=True)
    clip = jnp.maximum(1.0, jnp.sqrt(update_total / (M * D * FF)))
    factor = jnp.zeros((1, 128), F32)
    for m in range(M):
        own_factor = -(RATE * param_scale[m]) / clip * jnp.sqrt(row_mean[m])
        factor = factor + jnp.where(lax.rem(iota((1, 128), 1), 8) == m, own_factor, 0.0)
    r_out[...] = factor * jnp.sqrt(rnew[...])
    c_out[0:M, :] = jnp.sqrt(sel[0:M, :])

    arrive(rows_z)
    arrive(cols_z)
    for cp in own[M:]:
        cp.wait()
    arrive(par_copies)
    for cp in sent:
        cp.wait_send()


def apply_kernel(
    quarter, p_ref, s_ref, g_ref, r_ref, c_ref, rows_ref, cols_ref, map_ref,
    new_ref, change_ref, row_ref, col_ref,
):
    i = pl.program_id(0)
    m = i // quarter
    at = lax.rem(i, quarter)
    slots = 8 // quarter

    @pl.when(i == 0)
    def _():
        f = lax.axis_index(AXES)
        for n in range(M):
            b = map_ref[n, f]
            row_ref[n : n + 1, :] = rows_ref[b // 8, pl.ds(lax.rem(b, 8) * 8 + n, 1), 0:32]
            start = lax.rem(b, 16) * 80
            first = start // 128
            after = lax.min(first + 1, COLS // 128 - 1)
            pair = [cols_ref[a, b // 16, n : n + 1, :] for a in (first, after)]
            pair = jnp.broadcast_to(jnp.concatenate(pair, axis=1), (8, 256))
            take = jnp.where(iota((256, 128), 0) == start - first * 128 + iota((256, 128), 1), 1.0, 0.0)
            got = jnp.dot(pair, take, precision=HIGHEST, preferred_element_type=F32)
            col_ref[n : n + 1, :] = got[0:1, 0:80]

    lane = iota((ROWS, 128), 1)
    by_col = c_ref[pl.ds(m, 1), :]
    for s in range(slots):
        t = at * slots + s
        by_row = jnp.sum(jnp.where(lane == t * 8 + m, r_ref[...], 0.0), axis=1, keepdims=True)
        g = g_ref[t, m].astype(F32)
        change = (g * by_row) * by_col
        change_ref[0, s * ROWS : (s + 1) * ROWS, :] = change
        if CODED:
            step = s_ref[t, pl.ds(m, 1), :]
            step = jnp.concatenate([step] * (COLS // 256), axis=1)
            weights = p_ref[t, m].astype(jnp.int32).astype(F32) * step
        else:
            weights = p_ref[t, m]
        new_ref[0, s * ROWS : (s + 1) * ROWS, :] = weights + change


def shards(params, grads, row_state_old, col_state_old, old_map, new_map):
    vmem = pl.BlockSpec(memory_space=pltpu.VMEM)
    hbm = pl.BlockSpec(memory_space=pltpu.HBM)
    dma = pltpu.SemaphoreType.DMA
    given = (params, grads, row_state_old, col_state_old, old_map)
    held = [pltpu.with_memory_space_constraint(a, pltpu.HBM) for a in given]
    moved = pl.pallas_call(
        exchange_kernel,
        out_shape=[
            pltpu.VMEM((8, M, ROWS, COLS), jnp.int16 if CODED else F32),
            pltpu.VMEM((8, M, 256), F32),
            pltpu.VMEM((8, M, ROWS, COLS), jnp.bfloat16),
            pltpu.VMEM((ROWS, 128), F32),
            pltpu.VMEM((8, COLS), F32),
            pltpu.VMEM((16, 64, 128), F32),
            pltpu.VMEM((16, 8, 8, 128), F32),
        ],
        in_specs=[hbm] * 5,
        out_specs=[vmem] * 7,
        scratch_shapes=[
            pltpu.VMEM((M, ROWS, FF), jnp.bfloat16),
            pltpu.VMEM((M, ROWS, FF), F32),
            pltpu.VMEM((8, M, ROWS, COLS) if CODED else (8, M, 16, 128), jnp.int16),
            pltpu.VMEM((8, M, 256), F32),
            pltpu.VMEM((M, 32), F32),
            pltpu.VMEM((M, 80), F32),
            pltpu.VMEM((M, 128), jnp.int32),
            pltpu.VMEM((1024, 128), F32),
            pltpu.VMEM((128, 128), F32),
            pltpu.VMEM((4, 8, COLS), F32),
            pltpu.VMEM((4, 8, COLS), F32),
            pltpu.VMEM((4, 8, 128), F32),
            pltpu.VMEM((4, 8, 128), F32),
            pltpu.VMEM((128, COLS), F32),
            pltpu.VMEM((ROWS, 128), F32),
            dma((2 * M,)),
            dma((3,)),
            dma((2 * M + 1,)),
            dma((7,)), dma((7,)),
            dma((6,)), dma((6,)),
            dma((7,)), dma((7,)),
            dma((M + 1, 7)), dma((M + 1, 7)),
            dma((7,)), dma((7,)),
            dma((12,)), dma((12,)),
            dma((19,)), dma((19,)),
        ],
        compiler_params=pltpu.CompilerParams(
            collective_id=0, has_side_effects=True, vmem_limit_bytes=28 << 20
        ),
        name="exchange",
    )(*held)
    quarter = 4
    rows = 256 // quarter
    whole = pl.BlockSpec((1, rows, COLS), lambda i: (i // quarter, lax.rem(i, quarter), 0))
    return pl.pallas_call(
        functools.partial(apply_kernel, quarter),
        grid=(M * quarter,),
        out_shape=[
            jax.ShapeDtypeStruct((M, 256, COLS), F32),
            jax.ShapeDtypeStruct((M, 256, COLS), F32),
            jax.ShapeDtypeStruct((M, 32), F32),
            jax.ShapeDtypeStruct((M, 80), F32),
        ],
        in_specs=[vmem] * 7 + [pl.BlockSpec(memory_space=pltpu.SMEM)],
        out_specs=[
            whole,
            whole,
            pl.BlockSpec((M, 32), lambda i: (0, 0)),
            pl.BlockSpec((M, 80), lambda i: (0, 0)),
        ],
        compiler_params=pltpu.CompilerParams(vmem_limit_bytes=28 << 20),
        name="apply",
    )(*(pltpu.with_memory_space_constraint(a, pltpu.VMEM) for a in moved), new_map)


def solution(mesh):
    torus = Mesh(mesh.devices.reshape(4, 4, 4, 2), AXES)
    over = ("z", "y", "x", "c")
    return jax.shard_map(
        shards,
        mesh=torus,
        in_specs=(P(None, over, None), P(None, over, None), P(None, over), P(None, over), P(), P()),
        out_specs=(
            P(None, ("z", "y"), ("x", "c")),
            P(None, ("z", "y"), ("x", "c")),
            P(None, over),
            P(None, over),
        ),
        check_vma=False,
    )
```

```python
import functools
import math

import jax
import jax.numpy as jnp
from jax import lax
from jax.experimental import pallas as pl
from jax.experimental.pallas import tpu as pltpu
from jax.sharding import Mesh
from jax.sharding import PartitionSpec as P

D = 4096
FF = 10240
STEP = 4
M = 4
ROWS = 32
COLS = 1280
AXES = ("z", "y", "x", "c")
MESH = pl.DeviceIdType.MESH
HIGHEST = lax.Precision.HIGHEST
DECAY = 1.0 - float(STEP) ** (-0.8)
RATE = min(0.01, 1.0 / math.sqrt(STEP))
EPS = 1e-30
F32 = jnp.float32
TOP = 32767.0
CODED = True
FIRST = 2

COL_PEERS = [(1, 0), (3, 0), (2, 0), (1, 1), (3, 1), (2, 1), (0, 1)]
LINE_PEERS = [1, 2, 3]


def iota(shape, dim):
    return lax.broadcasted_iota(jnp.int32, shape, dim)


def exchange_kernel(
    params, grads, row_hbm, col_hbm, map_hbm,
    p_out, s_out, g_out, r_out, c_out, rows_out, cols_out,
    gv, pv, qv, sv, row_old, col_old, old_map, stored, row_tiles, red_y, red_z, sc_y, sc_z, sel, rnew,
    load_sem, small_sem, own_sem,
    s_tile, r_tile, s_line, r_line, s_grad, r_grad, s_par, r_par,
    s_row, r_row, s_red, r_red, s_sc, r_sc,
):
    z, y, x, c = (lax.axis_index(a) for a in AXES)
    k = x * 2 + c
    f = (z * 4 + y) * 8 + k

    def col_peer(i):
        dx, dc = COL_PEERS[i]
        return lax.rem(x + dx, 4), lax.rem(c + dc, 2)

    def to_cols(i, src, dst, ss, rs):
        tx, tc = col_peer(i)
        return pltpu.make_async_remote_copy(
            src_ref=src, dst_ref=dst, send_sem=ss, recv_sem=rs,
            device_id={"x": tx, "c": tc}, device_id_type=MESH,
        )

    def to_line(axis, d, src, dst, ss, rs):
        at = lax.rem((y if axis == "y" else z) + d, 4)
        return pltpu.make_async_remote_copy(
            src_ref=src, dst_ref=dst, send_sem=ss, recv_sem=rs,
            device_id={axis: at}, device_id_type=MESH,
        )

    def begin(copies):
        for cp in copies:
            cp.start()
        return copies

    def arrive(copies):
        for cp in copies:
            cp.wait_recv()

    small = [
        pltpu.make_async_copy(row_hbm, row_old, small_sem.at[0]),
        pltpu.make_async_copy(col_hbm, col_old, small_sem.at[1]),
        pltpu.make_async_copy(map_hbm, old_map, small_sem.at[2]),
    ]
    begin(small)
    loads = []
    for m in range(M):
        loads.append(pltpu.make_async_copy(grads.at[m], gv.at[m], load_sem.at[m]))
    for m in range(M):
        loads.append(pltpu.make_async_copy(params.at[m], pv.at[m], load_sem.at[M + m]))
    begin(loads)

    barrier = pltpu.get_barrier_semaphore()
    for i in range(7):
        tx, tc = col_peer(i)
        pl.semaphore_signal(barrier, inc=1, device_id={"x": tx, "c": tc}, device_id_type=MESH)
    for d in LINE_PEERS:
        pl.semaphore_signal(barrier, inc=1, device_id={"y": lax.rem(y + d, 4)}, device_id_type=MESH)
        pl.semaphore_signal(barrier, inc=1, device_id={"z": lax.rem(z + d, 4)}, device_id_type=MESH)

    mine = stored.at[pl.ds(pl.multiple_of(f * 8, 8), 8)]
    mine[...] = jnp.zeros((8, 128), F32)
    for cp in small:
        cp.wait()
    mine[0:4, 0:80] = col_old[...]
    mine[4:8, 0:32] = row_old[...]

    pl.semaphore_wait(barrier, 13)

    tiles = begin([to_cols(i, mine, mine, s_tile.at[i], r_tile.at[i]) for i in range(7)])
    sent = list(tiles)

    def columns(i):
        tx, tc = col_peer(i)
        return pl.ds(pl.multiple_of((tx * 2 + tc) * COLS, 128), COLS)

    grad_copies = begin(
        [to_cols(i, grads.at[:, :, columns(i)], g_out.at[k], s_grad.at[i], r_grad.at[i]) for i in range(7)]
    )
    sent += grad_copies

    def peer_block(i):
        tx, tc = col_peer(i)
        return tx * 2 + tc

    def send_params(m):
        if CODED:
            copies = [
                to_cols(i, qv.at[peer_block(i), m], p_out.at[k, m], s_par.at[m, i], r_par.at[m, i])
                for i in range(7)
            ]
        else:
            copies = [
                to_cols(i, params.at[m, :, columns(i)], p_out.at[k, m], s_par.at[m, i], r_par.at[m, i])
                for i in range(7)
            ]
        begin(copies)
        sent.extend(copies)
        return copies

    par_copies = []
    if not CODED:
        for m in range(FIRST):
            par_copies += send_params(m)

    own_columns = pl.ds(pl.multiple_of(k * COLS, 128), COLS)
    lane32 = iota((ROWS, 128), 1)
    row_sums = jnp.zeros((ROWS, 128), F32)
    own = []
    for m in range(M):
        loads[m].wait()

        def add_squares(t, acc, m=m):
            g = gv[m, :, pl.ds(pl.multiple_of(t * COLS, 128), COLS)].astype(F32)
            sq = g * g + EPS
            for u in range(COLS // 128):
                acc = acc + sq[:, u * 128 : (u + 1) * 128]
            return acc

        part = lax.fori_loop(0, 8, add_squares, jnp.zeros((ROWS, 128), F32))
        total = jnp.sum(part, axis=1, keepdims=True)
        row_sums = row_sums + jnp.where(lane32 == m, total, 0.0)
        own.append(pltpu.make_async_copy(gv.at[m, :, own_columns], g_out.at[k, m], own_sem.at[m]))
        own[-1].start()

    at8 = iota((8, 128), 0)
    lane8 = iota((8, 128), 1)
    squares = jnp.zeros((8, 128), F32)
    for m in range(M):
        loads[M + m].wait()

        def add_weights(t, acc, m=m):
            w = pv[m, :, pl.ds(pl.multiple_of(t * COLS, 128), COLS)]
            sq = w * w
            tops = [jnp.zeros((8, 128), F32)] * 2
            size = jnp.abs(w)
            for u in range(COLS // 128):
                for v in range(ROWS // 8):
                    acc = acc + sq[v * 8 : (v + 1) * 8, u * 128 : (u + 1) * 128]
                    if CODED:
                        tops[u % 2] = jnp.maximum(tops[u % 2], size[v * 8 : (v + 1) * 8, u * 128 : (u + 1) * 128])
            if CODED:
                top = jnp.concatenate([jnp.max(a, axis=0, keepdims=True) for a in tops], axis=1)
                top = jnp.maximum(top, 1e-30)
                sv[t, m : m + 1, :] = top * (1.0 / TOP)
                per = jnp.concatenate([TOP / top] * (COLS // 256), axis=1)
                qv[t, m] = jnp.round(w * per).astype(jnp.int32).astype(jnp.int16)
            return acc

        part = lax.fori_loop(0, 8, add_weights, jnp.zeros((8, 128), F32))
        total = jnp.sum(jnp.sum(part, axis=1, keepdims=True), axis=0, keepdims=True)
        squares = squares + jnp.where((at8 == m) & (lane8 == ROWS), total, 0.0)
        here = qv.at[k, m] if CODED else pv.at[m, :, own_columns]
        own.append(pltpu.make_async_copy(here, p_out.at[k, m], own_sem.at[M + m]))
        own[-1].start()
    if CODED:
        own.append(pltpu.make_async_copy(sv.at[k], s_out.at[k], own_sem.at[2 * M]))
        own[-1].start()
        par_copies += begin(
            [to_cols(i, sv.at[peer_block(i)], s_out.at[k], s_par.at[M, i], r_par.at[M, i]) for i in range(7)]
        )
        sent.extend(par_copies)
        for m in range(FIRST):
            par_copies += send_params(m)

    arrive(tiles)
    line_at = stored.at[pl.ds(pl.multiple_of((z * 4 + y) * 64, 64), 64)]
    lines = begin([to_line("y", d, line_at, line_at, s_line.at[d - 1], r_line.at[d - 1]) for d in LINE_PEERS])
    sent += lines

    arrive(lines)
    slab_at = stored.at[pl.ds(pl.multiple_of(z * 256, 256), 256)]
    slabs = begin([to_line("z", d, slab_at, slab_at, s_line.at[d + 2], r_line.at[d + 2]) for d in LINE_PEERS])
    sent += slabs
    arrive(slabs)

    at_row = iota((128, 128), 0)
    picked = jnp.zeros((128, 128), F32)
    for m in range(M):
        onehot = jnp.where((at_row == m) & (old_map[m : m + 1, :] == f), 1.0, 0.0)
        picked = picked + jnp.dot(
            onehot, stored[pl.ds(4 + m, 128, stride=8), :], precision=HIGHEST, preferred_element_type=F32
        )
    sel[...] = jnp.zeros((128, COLS), F32)
    sel[0:ROWS, 0:128] = row_sums
    row_sums = jnp.transpose(sel[:, 0:128])[0:8, :]
    row_new = DECAY * picked[0:8, :] + (1.0 - DECAY) * row_sums / FF
    row_new = jnp.where((at8 < M) & (lane8 < ROWS), row_new, 1.0)
    row_tiles[64:128, :] = jnp.ones((64, 128), F32)
    own_tile = row_tiles.at[pl.ds(pl.multiple_of(k * 8, 8), 8)]
    own_tile[...] = jnp.where(lane8 == ROWS, squares, row_new)
    row_copies = begin([to_cols(i, own_tile, own_tile, s_row.at[i], r_row.at[i]) for i in range(7)])
    sent += row_copies

    lane = iota((1, COLS), 1)
    block_of = ((lane.astype(F32) + 0.5) * (1.0 / 80.0)).astype(jnp.int32)
    place_of = lane - 80 * block_of
    at64 = iota((64, 128), 0)
    blocks = jnp.zeros((64, 128), F32)
    for m in range(M):
        wanted = (at64 - 16 * m) + k * 16
        inside = (at64 >= 16 * m) & (at64 < 16 * m + 16)
        onehot = jnp.where(inside & (old_map[m : m + 1, :] == wanted), 1.0, 0.0)
        blocks = blocks + jnp.dot(
            onehot, stored[pl.ds(m, 128, stride=8), :], precision=HIGHEST, preferred_element_type=F32
        )
    sel[0:64, 0:128] = blocks
    spread = jnp.where(iota((128, COLS), 0) == place_of, 1.0, 0.0)
    wide = jnp.dot(sel[0:64, 0:128], spread, precision=HIGHEST, preferred_element_type=F32)
    sel[0:64, :] = wide
    at16 = iota((16, COLS), 0)
    old_cols = [
        jnp.sum(jnp.where(at16 == block_of, sel[m * 16 : (m + 1) * 16, :], 0.0), axis=0, keepdims=True)
        for m in range(M)
    ]
    for m in range(M):
        c_out[m : m + 1, :] = old_cols[m]

    arrive(grad_copies)
    for m in range(M):
        own[m].wait()

    red_y[y, 4:8, :] = jnp.zeros((4, COLS), F32)
    for m in range(M):

        def add_columns(t, acc, m=m):
            g = g_out[t, m].astype(F32)
            sq = g * g + EPS
            for v in range(ROWS // 8):
                acc = acc + sq[v * 8 : (v + 1) * 8, :]
            return acc

        part = lax.fori_loop(0, 8, add_columns, jnp.zeros((8, COLS), F32))
        red_y[y, m : m + 1, :] = jnp.sum(part, axis=0, keepdims=True)

    arrive(row_copies)
    tile_sum = row_tiles[0:8, :]
    for t in range(1, 8):
        tile_sum = tile_sum + row_tiles[t * 8 : (t + 1) * 8, :]
    row_sum = jnp.sum(jnp.where(lane8 < ROWS, tile_sum, 0.0), axis=1, keepdims=True)
    weight_sum = jnp.sum(jnp.where(lane8 == ROWS, tile_sum, 0.0), axis=1, keepdims=True)
    both = jnp.where(lane8 == 0, row_sum, jnp.where(lane8 == 1, weight_sum, 0.0))
    red_y[y, 4:8, 0:128] = both[0:4, :]
    own_row = z * 4 + y
    rows_out[own_row] = row_tiles[0:64, :]

    stage = begin(
        [to_line("y", d, red_y.at[y], red_y.at[y], s_red.at[d - 1], r_red.at[d - 1]) for d in LINE_PEERS]
    )
    own_rows = rows_out.at[pl.ds(own_row, 1)]
    rows_y = begin(
        [to_line("y", d, own_rows, own_rows, s_red.at[d + 5], r_red.at[d + 5]) for d in LINE_PEERS]
    )
    arrive(stage)
    sent += stage + rows_y
    red_z[z] = red_y[0] + red_y[1] + red_y[2] + red_y[3]
    stage = begin(
        [to_line("z", d, red_z.at[z], red_z.at[z], s_red.at[d + 2], r_red.at[d + 2]) for d in LINE_PEERS]
    )
    arrive(rows_y)
    slab_rows = rows_out.at[pl.ds(pl.multiple_of(z * 4, 4), 4)]
    rows_z = begin(
        [to_line("z", d, slab_rows, slab_rows, s_red.at[d + 8], r_red.at[d + 8]) for d in LINE_PEERS]
    )
    arrive(stage)
    sent += stage + rows_z
    total = red_z[0] + red_z[1] + red_z[2] + red_z[3]

    row_mean = [total[4 + m : 5 + m, 0:1] / D for m in range(M)]
    param_scale = [jnp.sqrt(total[4 + m : 5 + m, 1:2] / (D * FF) + 1e-6) for m in range(M)]
    col_new = DECAY * c_out[0:M, :] + (1.0 - DECAY) * total[0:M, :] / D
    sel[0:M, :] = col_new
    piece = lax.min(own_row, COLS // 128 - 1)
    cols_out[own_row, k, 0:M, :] = sel[0:M, pl.ds(pl.multiple_of(piece * 128, 128), 128)]
    sel[0:M, :] = 1.0 / col_new
    new_rows = jnp.transpose(row_tiles[...])[0:ROWS, :]
    rnew[...] = 1.0 / new_rows

    update_sum = jnp.zeros((8, 128), F32)
    for m in range(M):
        inv_col = sel[m : m + 1, :]

        def add_updates(t, acc, m=m, inv_col=inv_col):
            g = g_out[t, m].astype(F32)
            sq = g * g * inv_col
            part = sq[:, 0:128]
            for u in range(1, COLS // 128):
                part = part + sq[:, u * 128 : (u + 1) * 128]
            part = part * jnp.sum(jnp.where(lane32 == t * 8 + m, rnew[...], 0.0), axis=1, keepdims=True)
            for v in range(ROWS // 8):
                acc = acc + part[v * 8 : (v + 1) * 8, :]
            return acc

        part = lax.fori_loop(0, 8, add_updates, jnp.zeros((8, 128), F32))
        update_sum = update_sum + part * row_mean[m]
    cols_out[own_row, k, 4:8, :] = update_sum[0:4, :] + update_sum[4:8, :]
    own_col = cols_out.at[own_row, k]
    sums = begin([to_cols(i, own_col, own_col, s_sc.at[i], r_sc.at[i]) for i in range(7)])
    sent += sums

    for m in range(FIRST, M):
        par_copies += send_params(m)

    arrive(sums)
    update_sum = cols_out[own_row, 0, 4:8, :]
    for t in range(1, 8):
        update_sum = update_sum + cols_out[own_row, t, 4:8, :]
    sc_y[y] = jnp.zeros((8, 128), F32)
    sc_y[y, 0:4, :] = update_sum
    stage = begin(
        [to_line("y", d, sc_y.at[y], sc_y.at[y], s_sc.at[d + 6], r_sc.at[d + 6]) for d in LINE_PEERS]
    )
    own_cols = cols_out.at[pl.ds(own_row, 1)]
    cols_y = begin(
        [to_line("y", d, own_cols, own_cols, s_sc.at[d + 12], r_sc.at[d + 12]) for d in LINE_PEERS]
    )
    arrive(stage)
    sent += stage + cols_y
    sc_z[z] = sc_y[0] + sc_y[1] + sc_y[2] + sc_y[3]
    stage = begin(
        [to_line("z", d, sc_z.at[z], sc_z.at[z], s_sc.at[d + 9], r_sc.at[d + 9]) for d in LINE_PEERS]
    )
    arrive(cols_y)
    slab_cols = cols_out.at[pl.ds(pl.multiple_of(z * 4, 4), 4)]
    cols_z = begin(
        [to_line("z", d, slab_cols, slab_cols, s_sc.at[d + 15], r_sc.at[d + 15]) for d in LINE_PEERS]
    )
    arrive(stage)
    sent += stage + cols_z
    update_sum = sc_z[0] + sc_z[1] + sc_z[2] + sc_z[3]
    update_total = jnp.sum(jnp.sum(update_sum, axis=1, keepdims=True), axis=0, keepdims=True)
    clip = jnp.maximum(1.0, jnp.sqrt(update_total / (M * D * FF)))
    factor = jnp.zeros((1, 128), F32)
    for m in range(M):
        own_factor = -(RATE * param_scale[m]) / clip * jnp.sqrt(row_mean[m])
        factor = factor + jnp.where(lax.rem(iota((1, 128), 1), 8) == m, own_factor, 0.0)
    r_out[...] = factor * jnp.sqrt(rnew[...])
    c_out[0:M, :] = jnp.sqrt(sel[0:M, :])

    arrive(rows_z)
    arrive(cols_z)
    for cp in own[M:]:
        cp.wait()
    arrive(par_copies)
    for cp in sent:
        cp.wait_send()


def apply_kernel(
    quarter, p_ref, s_ref, g_ref, r_ref, c_ref, rows_ref, cols_ref, map_ref,
    new_ref, change_ref, row_ref, col_ref,
):
    i = pl.program_id(0)
    m = i // quarter
    at = lax.rem(i, quarter)
    slots = 8 // quarter

    @pl.when(i == 0)
    def _():
        f = lax.axis_index(AXES)
        for n in range(M):
            b = map_ref[n, f]
            row_ref[n : n + 1, :] = rows_ref[b // 8, pl.ds(lax.rem(b, 8) * 8 + n, 1), 0:32]
            start = lax.rem(b, 16) * 80
            first = start // 128
            after = lax.min(first + 1, COLS // 128 - 1)
            pair = [cols_ref[a, b // 16, n : n + 1, :] for a in (first, after)]
            pair = jnp.broadcast_to(jnp.concatenate(pair, axis=1), (8, 256))
            take = jnp.where(iota((256, 128), 0) == start - first * 128 + iota((256, 128), 1), 1.0, 0.0)
            got = jnp.dot(pair, take, precision=HIGHEST, preferred_element_type=F32)
            col_ref[n : n + 1, :] = got[0:1, 0:80]

    lane = iota((ROWS, 128), 1)
    by_col = c_ref[pl.ds(m, 1), :]
    for s in range(slots):
        t = at * slots + s
        by_row = jnp.sum(jnp.where(lane == t * 8 + m, r_ref[...], 0.0), axis=1, keepdims=True)
        g = g_ref[t, m].astype(F32)
        change = (g * by_row) * by_col
        change_ref[0, s * ROWS : (s + 1) * ROWS, :] = change
        if CODED:
            step = s_ref[t, pl.ds(m, 1), :]
            step = jnp.concatenate([step] * (COLS // 256), axis=1)
            weights = p_ref[t, m].astype(jnp.int32).astype(F32) * step
        else:
            weights = p_ref[t, m]
        new_ref[0, s * ROWS : (s + 1) * ROWS, :] = weights + change


def shards(params, grads, row_state_old, col_state_old, old_map, new_map):
    vmem = pl.BlockSpec(memory_space=pltpu.VMEM)
    hbm = pl.BlockSpec(memory_space=pltpu.HBM)
    dma = pltpu.SemaphoreType.DMA
    given = (params, grads, row_state_old, col_state_old, old_map)
    held = [pltpu.with_memory_space_constraint(a, pltpu.HBM) for a in given]
    moved = pl.pallas_call(
        exchange_kernel,
        out_shape=[
            pltpu.VMEM((8, M, ROWS, COLS), jnp.int16 if CODED else F32),
            pltpu.VMEM((8, M, 256), F32),
            pltpu.VMEM((8, M, ROWS, COLS), jnp.bfloat16),
            pltpu.VMEM((ROWS, 128), F32),
            pltpu.VMEM((8, COLS), F32),
            pltpu.VMEM((16, 64, 128), F32),
            pltpu.VMEM((16, 8, 8, 128), F32),
        ],
        in_specs=[hbm] * 5,
        out_specs=[vmem] * 7,
        scratch_shapes=[
            pltpu.VMEM((M, ROWS, FF), jnp.bfloat16),
            pltpu.VMEM((M, ROWS, FF), F32),
            pltpu.VMEM((8, M, ROWS, COLS) if CODED else (8, M, 16, 128), jnp.int16),
            pltpu.VMEM((8, M, 256), F32),
            pltpu.VMEM((M, 32), F32),
            pltpu.VMEM((M, 80), F32),
            pltpu.VMEM((M, 128), jnp.int32),
            pltpu.VMEM((1024, 128), F32),
            pltpu.VMEM((128, 128), F32),
            pltpu.VMEM((4, 8, COLS), F32),
            pltpu.VMEM((4, 8, COLS), F32),
            pltpu.VMEM((4, 8, 128), F32),
            pltpu.VMEM((4, 8, 128), F32),
            pltpu.VMEM((128, COLS), F32),
            pltpu.VMEM((ROWS, 128), F32),
            dma((2 * M,)),
            dma((3,)),
            dma((2 * M + 1,)),
            dma((7,)), dma((7,)),
            dma((6,)), dma((6,)),
            dma((7,)), dma((7,)),
            dma((M + 1, 7)), dma((M + 1, 7)),
            dma((7,)), dma((7,)),
            dma((12,)), dma((12,)),
            dma((19,)), dma((19,)),
        ],
        compiler_params=pltpu.CompilerParams(
            collective_id=0, has_side_effects=True, vmem_limit_bytes=28 << 20
        ),
        name="exchange",
    )(*held)
    quarter = 4
    rows = 256 // quarter
    whole = pl.BlockSpec((1, rows, COLS), lambda i: (i // quarter, lax.rem(i, quarter), 0))
    return pl.pallas_call(
        functools.partial(apply_kernel, quarter),
        grid=(M * quarter,),
        out_shape=[
            jax.ShapeDtypeStruct((M, 256, COLS), F32),
            jax.ShapeDtypeStruct((M, 256, COLS), F32),
            jax.ShapeDtypeStruct((M, 32), F32),
            jax.ShapeDtypeStruct((M, 80), F32),
        ],
        in_specs=[vmem] * 7 + [pl.BlockSpec(memory_space=pltpu.SMEM)],
        out_specs=[
            whole,
            whole,
            pl.BlockSpec((M, 32), lambda i: (0, 0)),
            pl.BlockSpec((M, 80), lambda i: (0, 0)),
        ],
        compiler_params=pltpu.CompilerParams(vmem_limit_bytes=28 << 20),
        name="apply",
    )(*(pltpu.with_memory_space_constraint(a, pltpu.VMEM) for a in moved), new_map)


def solution(mesh):
    torus = Mesh(mesh.devices.reshape(4, 4, 4, 2), AXES)
    over = ("z", "y", "x", "c")
    return jax.shard_map(
        shards,
        mesh=torus,
        in_specs=(P(None, over, None), P(None, over, None), P(None, over), P(None, over), P(), P()),
        out_specs=(
            P(None, ("z", "y"), ("x", "c")),
            P(None, ("z", "y"), ("x", "c")),
            P(None, over),
            P(None, over),
        ),
        check_vma=False,
    )
```

```python
import math

import jax
import jax.numpy as jnp
from jax import lax
from jax.experimental import pallas as pl
from jax.experimental.pallas import tpu as pltpu
from jax.sharding import Mesh
from jax.sharding import PartitionSpec as P

D = 4096
FF = 10240
STEP = 4
M = 4
ROWS = 32
COLS = 1280
AXES = ("z", "y", "x", "c")
MESH = pl.DeviceIdType.MESH
HIGHEST = lax.Precision.HIGHEST
DECAY = 1.0 - float(STEP) ** (-0.8)
RATE = min(0.01, 1.0 / math.sqrt(STEP))
EPS = 1e-30
F32 = jnp.float32
TOP = 32767.0
CODED = True
PIECE = 3
FIRST = 2

COL_PEERS = [(1, 0), (3, 0), (2, 0), (1, 1), (3, 1), (2, 1), (0, 1)]
LINE_PEERS = [1, 2, 3]


def iota(shape, dim):
    return lax.broadcasted_iota(jnp.int32, shape, dim)


def exchange_kernel(
    params, grads, row_hbm, col_hbm, map_hbm,
    p_out, s_out, g_out, r_out, c_out, rows_out, cols_out,
    gv, pv, qv, sv, row_old, col_old, old_map, stored, row_tiles, red_y, red_z, sc_x, sc_y, sc_z, sel, rnew,
    load_sem, small_sem, own_sem,
    s_tile, r_tile, s_line, r_line, s_grad, r_grad, s_par, r_par,
    s_row, r_row, s_red, r_red, s_sc, r_sc, s_col, r_col,
):
    z, y, x, c = (lax.axis_index(a) for a in AXES)
    k = x * 2 + c
    f = (z * 4 + y) * 8 + k

    def col_peer(i):
        dx, dc = COL_PEERS[i]
        return lax.rem(x + dx, 4), lax.rem(c + dc, 2)

    def to_cols(i, src, dst, ss, rs):
        tx, tc = col_peer(i)
        return pltpu.make_async_remote_copy(
            src_ref=src, dst_ref=dst, send_sem=ss, recv_sem=rs,
            device_id={"x": tx, "c": tc}, device_id_type=MESH,
        )

    def to_line(axis, d, src, dst, ss, rs):
        at = lax.rem((y if axis == "y" else z) + d, 4)
        return pltpu.make_async_remote_copy(
            src_ref=src, dst_ref=dst, send_sem=ss, recv_sem=rs,
            device_id={axis: at}, device_id_type=MESH,
        )

    def begin(copies):
        for cp in copies:
            cp.start()
        return copies

    def arrive(copies):
        for cp in copies:
            cp.wait_recv()

    small = [
        pltpu.make_async_copy(row_hbm, row_old, small_sem.at[0]),
        pltpu.make_async_copy(col_hbm, col_old, small_sem.at[1]),
        pltpu.make_async_copy(map_hbm, old_map, small_sem.at[2]),
    ]
    begin(small)
    loads = []
    for m in range(M):
        loads.append(pltpu.make_async_copy(grads.at[m], gv.at[m], load_sem.at[m]))
    for m in range(M):
        loads.append(pltpu.make_async_copy(params.at[m], pv.at[m], load_sem.at[M + m]))
    begin(loads)

    barrier = pltpu.get_barrier_semaphore()
    for i in range(7):
        tx, tc = col_peer(i)
        pl.semaphore_signal(barrier, inc=1, device_id={"x": tx, "c": tc}, device_id_type=MESH)
    for d in LINE_PEERS:
        pl.semaphore_signal(barrier, inc=1, device_id={"y": lax.rem(y + d, 4)}, device_id_type=MESH)
        pl.semaphore_signal(barrier, inc=1, device_id={"z": lax.rem(z + d, 4)}, device_id_type=MESH)

    mine = stored.at[pl.ds(pl.multiple_of(f * 8, 8), 8)]
    mine[...] = jnp.zeros((8, 128), F32)
    for cp in small:
        cp.wait()
    mine[0:4, 0:80] = col_old[...]
    mine[4:8, 0:32] = row_old[...]

    pl.semaphore_wait(barrier, 13)

    tiles = begin([to_cols(i, mine, mine, s_tile.at[i], r_tile.at[i]) for i in range(7)])
    sent = list(tiles)

    def columns(i):
        tx, tc = col_peer(i)
        return pl.ds(pl.multiple_of((tx * 2 + tc) * COLS, 128), COLS)

    grad_copies = begin(
        [to_cols(i, grads.at[:, :, columns(i)], g_out.at[k], s_grad.at[i], r_grad.at[i]) for i in range(7)]
    )
    sent += grad_copies

    def peer_block(i):
        tx, tc = col_peer(i)
        return tx * 2 + tc

    def send_params(m):
        if CODED:
            copies = [
                to_cols(i, qv.at[peer_block(i), m], p_out.at[k, m], s_par.at[m, i], r_par.at[m, i])
                for i in range(7)
            ]
        else:
            copies = [
                to_cols(i, params.at[m, :, columns(i)], p_out.at[k, m], s_par.at[m, i], r_par.at[m, i])
                for i in range(7)
            ]
        begin(copies)
        sent.extend(copies)
        return copies

    par_copies = []

    own_columns = pl.ds(pl.multiple_of(k * COLS, 128), COLS)
    lane32 = iota((ROWS, 128), 1)
    row_sums = jnp.zeros((ROWS, 128), F32)
    own = []
    for m in range(M):
        loads[m].wait()

        def add_squares(t, acc, m=m):
            g = gv[m, :, pl.ds(pl.multiple_of(t * COLS, 128), COLS)].astype(F32)
            sq = g * g + EPS
            for u in range(COLS // 128):
                acc = acc + sq[:, u * 128 : (u + 1) * 128]
            return acc

        part = lax.fori_loop(0, 8, add_squares, jnp.zeros((ROWS, 128), F32))
        total = jnp.sum(part, axis=1, keepdims=True)
        row_sums = row_sums + jnp.where(lane32 == m, total, 0.0)
        own.append(pltpu.make_async_copy(gv.at[m, :, own_columns], g_out.at[k, m], own_sem.at[m]))
        own[-1].start()

    at8 = iota((8, 128), 0)
    lane8 = iota((8, 128), 1)
    squares = jnp.zeros((8, 128), F32)
    for m in range(M):
        loads[M + m].wait()

        def add_weights(t, acc, m=m):
            w = pv[m, :, pl.ds(pl.multiple_of(t * COLS, 128), COLS)]
            sq = w * w
            tops = [jnp.zeros((8, 128), F32)] * 2
            size = jnp.abs(w)
            for u in range(COLS // 128):
                for v in range(ROWS // 8):
                    acc = acc + sq[v * 8 : (v + 1) * 8, u * 128 : (u + 1) * 128]
                    if CODED:
                        tops[u % 2] = jnp.maximum(tops[u % 2], size[v * 8 : (v + 1) * 8, u * 128 : (u + 1) * 128])
            if CODED:
                top = jnp.concatenate([jnp.max(a, axis=0, keepdims=True) for a in tops], axis=1)
                top = jnp.maximum(top, 1e-30)
                sv[t, m : m + 1, :] = top * (1.0 / TOP)
                per = jnp.concatenate([TOP / top] * (COLS // 256), axis=1)
                qv[t, m] = jnp.round(w * per).astype(jnp.int32).astype(jnp.int16)
            return acc

        part = lax.fori_loop(0, 8, add_weights, jnp.zeros((8, 128), F32))
        total = jnp.sum(jnp.sum(part, axis=1, keepdims=True), axis=0, keepdims=True)
        squares = squares + jnp.where((at8 == m) & (lane8 == ROWS), total, 0.0)
        here = qv.at[k, m] if CODED else pv.at[m, :, own_columns]
        own.append(pltpu.make_async_copy(here, p_out.at[k, m], own_sem.at[M + m]))
        own[-1].start()
    if CODED:
        own.append(pltpu.make_async_copy(sv.at[k], s_out.at[k], own_sem.at[2 * M]))
        own[-1].start()
        par_copies += begin(
            [to_cols(i, sv.at[peer_block(i)], s_out.at[k], s_par.at[M, i], r_par.at[M, i]) for i in range(7)]
        )
        sent.extend(par_copies)

    arrive(tiles)
    line_at = stored.at[pl.ds(pl.multiple_of((z * 4 + y) * 64, 64), 64)]
    lines = begin([to_line("y", d, line_at, line_at, s_line.at[d - 1], r_line.at[d - 1]) for d in LINE_PEERS])
    sent += lines

    arrive(lines)
    slab_at = stored.at[pl.ds(pl.multiple_of(z * 256, 256), 256)]
    slabs = begin([to_line("z", d, slab_at, slab_at, s_line.at[d + 2], r_line.at[d + 2]) for d in LINE_PEERS])
    sent += slabs
    arrive(slabs)

    at_row = iota((128, 128), 0)
    picked = jnp.zeros((128, 128), F32)
    for m in range(M):
        onehot = jnp.where((at_row == m) & (old_map[m : m + 1, :] == f), 1.0, 0.0)
        picked = picked + jnp.dot(
            onehot, stored[pl.ds(4 + m, 128, stride=8), :], precision=HIGHEST, preferred_element_type=F32
        )
    sel[...] = jnp.zeros((128, COLS), F32)
    sel[0:ROWS, 0:128] = row_sums
    row_sums = jnp.transpose(sel[:, 0:128])[0:8, :]
    row_new = DECAY * picked[0:8, :] + (1.0 - DECAY) * row_sums / FF
    row_new = jnp.where((at8 < M) & (lane8 < ROWS), row_new, 1.0)
    row_tiles[64:128, :] = jnp.ones((64, 128), F32)
    own_tile = row_tiles.at[pl.ds(pl.multiple_of(k * 8, 8), 8)]
    own_tile[...] = jnp.where(lane8 == ROWS, squares, row_new)
    row_copies = begin([to_cols(i, own_tile, own_tile, s_row.at[i], r_row.at[i]) for i in range(7)])
    sent += row_copies
    for m in range(FIRST):
        par_copies += send_params(m)

    lane = iota((1, COLS), 1)
    block_of = ((lane.astype(F32) + 0.5) * (1.0 / 80.0)).astype(jnp.int32)
    place_of = lane - 80 * block_of
    at64 = iota((64, 128), 0)
    blocks = jnp.zeros((64, 128), F32)
    for m in range(M):
        wanted = (at64 - 16 * m) + k * 16
        inside = (at64 >= 16 * m) & (at64 < 16 * m + 16)
        onehot = jnp.where(inside & (old_map[m : m + 1, :] == wanted), 1.0, 0.0)
        blocks = blocks + jnp.dot(
            onehot, stored[pl.ds(m, 128, stride=8), :], precision=HIGHEST, preferred_element_type=F32
        )
    sel[0:64, 0:128] = blocks
    spread = jnp.where(iota((128, COLS), 0) == place_of, 1.0, 0.0)
    wide = jnp.dot(sel[0:64, 0:128], spread, precision=HIGHEST, preferred_element_type=F32)
    sel[0:64, :] = wide
    at16 = iota((16, COLS), 0)
    old_cols = [
        jnp.sum(jnp.where(at16 == block_of, sel[m * 16 : (m + 1) * 16, :], 0.0), axis=0, keepdims=True)
        for m in range(M)
    ]
    for m in range(M):
        c_out[m : m + 1, :] = old_cols[m]

    arrive(grad_copies)
    for m in range(M):
        own[m].wait()

    red_y[y, 4:8, :] = jnp.zeros((4, COLS), F32)
    for m in range(M):

        def add_columns(t, acc, m=m):
            g = g_out[t, m].astype(F32)
            sq = g * g + EPS
            for v in range(ROWS // 8):
                acc = acc + sq[v * 8 : (v + 1) * 8, :]
            return acc

        part = lax.fori_loop(0, 8, add_columns, jnp.zeros((8, COLS), F32))
        red_y[y, m : m + 1, :] = jnp.sum(part, axis=0, keepdims=True)

    arrive(row_copies)
    tile_sum = row_tiles[0:8, :]
    for t in range(1, 8):
        tile_sum = tile_sum + row_tiles[t * 8 : (t + 1) * 8, :]
    row_sum = jnp.sum(jnp.where(lane8 < ROWS, tile_sum, 0.0), axis=1, keepdims=True)
    weight_sum = jnp.sum(jnp.where(lane8 == ROWS, tile_sum, 0.0), axis=1, keepdims=True)
    both = jnp.where(lane8 == 0, row_sum, jnp.where(lane8 == 1, weight_sum, 0.0))
    red_y[y, 4:8, 0:128] = both[0:4, :]
    own_row = z * 4 + y
    rows_out[own_row] = row_tiles[0:64, :]

    stage = begin(
        [to_line("y", d, red_y.at[y], red_y.at[y], s_red.at[d - 1], r_red.at[d - 1]) for d in LINE_PEERS]
    )
    own_rows = rows_out.at[pl.ds(own_row, 1)]
    rows_y = begin(
        [to_line("y", d, own_rows, own_rows, s_red.at[d + 5], r_red.at[d + 5]) for d in LINE_PEERS]
    )
    arrive(stage)
    sent += stage + rows_y
    red_z[z] = red_y[0] + red_y[1] + red_y[2] + red_y[3]
    stage = begin(
        [to_line("z", d, red_z.at[z], red_z.at[z], s_red.at[d + 2], r_red.at[d + 2]) for d in LINE_PEERS]
    )
    arrive(rows_y)
    slab_rows = rows_out.at[pl.ds(pl.multiple_of(z * 4, 4), 4)]
    rows_z = begin(
        [to_line("z", d, slab_rows, slab_rows, s_red.at[d + 8], r_red.at[d + 8]) for d in LINE_PEERS]
    )
    arrive(stage)
    sent += stage + rows_z
    total = red_z[0] + red_z[1] + red_z[2] + red_z[3]

    row_mean = [total[4 + m : 5 + m, 0:1] / D for m in range(M)]
    param_scale = [jnp.sqrt(total[4 + m : 5 + m, 1:2] / (D * FF) + 1e-6) for m in range(M)]
    col_new = DECAY * c_out[0:M, :] + (1.0 - DECAY) * total[0:M, :] / D
    sel[0:M, :] = col_new
    piece = lax.min(y * PIECE, COLS // 128 - PIECE)
    cols_out[y, k] = sel[0:M, pl.ds(pl.multiple_of(piece * 128, 128), PIECE * 128)]
    sel[0:M, :] = 1.0 / col_new
    new_rows = jnp.transpose(row_tiles[...])[0:ROWS, :]
    rnew[...] = 1.0 / new_rows

    update_sum = jnp.zeros((8, 128), F32)
    for m in range(M):
        inv_col = sel[m : m + 1, :]

        def add_updates(t, acc, m=m, inv_col=inv_col):
            g = g_out[t, m].astype(F32)
            sq = g * g * inv_col
            part = sq[:, 0:128]
            for u in range(1, COLS // 128):
                part = part + sq[:, u * 128 : (u + 1) * 128]
            part = part * jnp.sum(jnp.where(lane32 == t * 8 + m, rnew[...], 0.0), axis=1, keepdims=True)
            for v in range(ROWS // 8):
                acc = acc + part[v * 8 : (v + 1) * 8, :]
            return acc

        part = lax.fori_loop(0, 8, add_updates, jnp.zeros((8, 128), F32))
        update_sum = update_sum + part * row_mean[m]
    sc_x[k] = update_sum
    sums = begin([to_cols(i, sc_x.at[k], sc_x.at[k], s_sc.at[i], r_sc.at[i]) for i in range(7)])
    own_col = cols_out.at[y, k]
    cols_x = begin([to_cols(i, own_col, own_col, s_col.at[i], r_col.at[i]) for i in range(7)])
    sent += sums + cols_x

    for m in range(FIRST, M):
        par_copies += send_params(m)

    arrive(sums)
    update_sum = sc_x[0]
    for t in range(1, 8):
        update_sum = update_sum + sc_x[t]
    sc_y[y] = update_sum
    stage = begin(
        [to_line("y", d, sc_y.at[y], sc_y.at[y], s_sc.at[d + 6], r_sc.at[d + 6]) for d in LINE_PEERS]
    )
    arrive(cols_x)
    own_cols = cols_out.at[pl.ds(y, 1)]
    cols_y = begin(
        [to_line("y", d, own_cols, own_cols, s_col.at[d + 6], r_col.at[d + 6]) for d in LINE_PEERS]
    )
    arrive(stage)
    sent += stage + cols_y
    sc_z[z] = sc_y[0] + sc_y[1] + sc_y[2] + sc_y[3]
    stage = begin(
        [to_line("z", d, sc_z.at[z], sc_z.at[z], s_sc.at[d + 9], r_sc.at[d + 9]) for d in LINE_PEERS]
    )
    arrive(stage)
    sent += stage
    update_sum = sc_z[0] + sc_z[1] + sc_z[2] + sc_z[3]
    update_total = jnp.sum(jnp.sum(update_sum, axis=1, keepdims=True), axis=0, keepdims=True)
    clip = jnp.maximum(1.0, jnp.sqrt(update_total / (M * D * FF)))
    factor = jnp.zeros((1, 128), F32)
    for m in range(M):
        own_factor = -(RATE * param_scale[m]) / clip * jnp.sqrt(row_mean[m])
        factor = factor + jnp.where(lax.rem(iota((1, 128), 1), 8) == m, own_factor, 0.0)
    r_out[...] = factor * jnp.sqrt(rnew[...])
    c_out[0:M, :] = jnp.sqrt(sel[0:M, :])

    arrive(rows_z)
    arrive(cols_y)
    for cp in own[M:]:
        cp.wait()
    arrive(par_copies)
    for cp in sent:
        cp.wait_send()


def apply_kernel(
    p_ref, s_ref, g_ref, r_ref, c_ref, rows_ref, cols_ref, map_hbm,
    new_hbm, change_hbm, row_hbm, col_hbm,
    new_buf, change_buf, row_buf, col_buf, new_map, big_sem, small_sem,
):
    fetch = pltpu.make_async_copy(map_hbm, new_map, small_sem.at[0])
    fetch.start()
    lane = iota((ROWS, 128), 1)

    def stores(m, t):
        rows = pl.ds(pl.multiple_of(t * ROWS, ROWS), ROWS)
        return [
            pltpu.make_async_copy(change_buf.at[m, rows], change_hbm.at[m, rows], big_sem.at[0, m, t]),
            pltpu.make_async_copy(new_buf.at[m, rows], new_hbm.at[m, rows], big_sem.at[1, m, t]),
        ]

    for m in range(M):
        by_col = c_ref[m : m + 1, :]

        def block(t, carry, m=m, by_col=by_col):
            rows = pl.ds(pl.multiple_of(t * ROWS, ROWS), ROWS)
            by_row = jnp.sum(jnp.where(lane == t * 8 + m, r_ref[...], 0.0), axis=1, keepdims=True)
            g = g_ref[t, m].astype(F32)
            change = (g * by_row) * by_col
            change_buf[m, rows, :] = change
            if CODED:
                step = jnp.concatenate([s_ref[t, m : m + 1, :]] * (COLS // 256), axis=1)
                weights = p_ref[t, m].astype(jnp.int32).astype(F32) * step
            else:
                weights = p_ref[t, m]
            new_buf[m, rows, :] = weights + change
            for cp in stores(m, t):
                cp.start()
            return carry

        lax.fori_loop(0, 8, block, 0)

    fetch.wait()
    f = lax.axis_index(AXES)
    for n in range(M):
        b = new_map[n, f]
        row_buf[n : n + 1, :] = rows_ref[b // 8, pl.ds(lax.rem(b, 8) * 8 + n, 1), 0:32]
        start = lax.rem(b, 16) * 80
        first = start // 128
        pair = []
        for t in (first, lax.min(first + 1, COLS // 128 - 1)):
            piece = lax.min(t // PIECE, 3)
            at = t - lax.min(piece * PIECE, COLS // 128 - PIECE)
            pair.append(cols_ref[piece, b // 16, n : n + 1, pl.ds(pl.multiple_of(at * 128, 128), 128)])
        pair = jnp.broadcast_to(jnp.concatenate(pair, axis=1), (8, 256))
        take = jnp.where(iota((256, 128), 0) == start - first * 128 + iota((256, 128), 1), 1.0, 0.0)
        got = jnp.dot(pair, take, precision=HIGHEST, preferred_element_type=F32)
        col_buf[n : n + 1, :] = got[0:1, 0:80]
    small = [
        pltpu.make_async_copy(row_buf, row_hbm, small_sem.at[1]),
        pltpu.make_async_copy(col_buf, col_hbm, small_sem.at[2]),
    ]
    for cp in small:
        cp.start()

    for m in range(M):

        def finish(t, carry, m=m):
            for cp in stores(m, t):
                cp.wait()
            return carry

        lax.fori_loop(0, 8, finish, 0)
    for cp in small:
        cp.wait()


def shards(params, grads, row_state_old, col_state_old, old_map, new_map):
    vmem = pl.BlockSpec(memory_space=pltpu.VMEM)
    hbm = pl.BlockSpec(memory_space=pltpu.HBM)
    dma = pltpu.SemaphoreType.DMA
    given = (params, grads, row_state_old, col_state_old, old_map)
    held = [pltpu.with_memory_space_constraint(a, pltpu.HBM) for a in given]
    held_map = pltpu.with_memory_space_constraint(new_map, pltpu.HBM)
    moved = pl.pallas_call(
        exchange_kernel,
        out_shape=[
            pltpu.VMEM((8, M, ROWS, COLS), jnp.int16 if CODED else F32),
            pltpu.VMEM((8, M, 256), F32),
            pltpu.VMEM((8, M, ROWS, COLS), jnp.bfloat16),
            pltpu.VMEM((ROWS, 128), F32),
            pltpu.VMEM((8, COLS), F32),
            pltpu.VMEM((16, 64, 128), F32),
            pltpu.VMEM((4, 8, M, PIECE * 128), F32),
        ],
        in_specs=[hbm] * 5,
        out_specs=[vmem] * 7,
        scratch_shapes=[
            pltpu.VMEM((M, ROWS, FF), jnp.bfloat16),
            pltpu.VMEM((M, ROWS, FF), F32),
            pltpu.VMEM((8, M, ROWS, COLS) if CODED else (8, M, 16, 128), jnp.int16),
            pltpu.VMEM((8, M, 256), F32),
            pltpu.VMEM((M, 32), F32),
            pltpu.VMEM((M, 80), F32),
            pltpu.VMEM((M, 128), jnp.int32),
            pltpu.VMEM((1024, 128), F32),
            pltpu.VMEM((128, 128), F32),
            pltpu.VMEM((4, 8, COLS), F32),
            pltpu.VMEM((4, 8, COLS), F32),
            pltpu.VMEM((8, 8, 128), F32),
            pltpu.VMEM((4, 8, 128), F32),
            pltpu.VMEM((4, 8, 128), F32),
            pltpu.VMEM((128, COLS), F32),
            pltpu.VMEM((ROWS, 128), F32),
            dma((2 * M,)),
            dma((3,)),
            dma((2 * M + 1,)),
            dma((7,)), dma((7,)),
            dma((6,)), dma((6,)),
            dma((7,)), dma((7,)),
            dma((M + 1, 7)), dma((M + 1, 7)),
            dma((7,)), dma((7,)),
            dma((12,)), dma((12,)),
            dma((13,)), dma((13,)),
            dma((10,)), dma((10,)),
        ],
        compiler_params=pltpu.CompilerParams(
            collective_id=0, has_side_effects=True, vmem_limit_bytes=28 << 20
        ),
        name="exchange",
    )(*held)
    return pl.pallas_call(
        apply_kernel,
        out_shape=[
            jax.ShapeDtypeStruct((M, 256, COLS), F32),
            jax.ShapeDtypeStruct((M, 256, COLS), F32),
            jax.ShapeDtypeStruct((M, 32), F32),
            jax.ShapeDtypeStruct((M, 80), F32),
        ],
        in_specs=[vmem] * 7 + [hbm],
        out_specs=[hbm] * 4,
        scratch_shapes=[
            pltpu.VMEM((M, 256, COLS), F32),
            pltpu.VMEM((M, 256, COLS), F32),
            pltpu.VMEM((M, 32), F32),
            pltpu.VMEM((M, 80), F32),
            pltpu.SMEM((M, 128), jnp.int32),
            dma((2, M, 8)),
            dma((3,)),
        ],
        compiler_params=pltpu.CompilerParams(vmem_limit_bytes=28 << 20),
        name="apply",
    )(*(pltpu.with_memory_space_constraint(a, pltpu.VMEM) for a in moved), held_map)


def solution(mesh):
    torus = Mesh(mesh.devices.reshape(4, 4, 4, 2), AXES)
    over = ("z", "y", "x", "c")
    return jax.shard_map(
        shards,
        mesh=torus,
        in_specs=(P(None, over, None), P(None, over, None), P(None, over), P(None, over), P(), P()),
        out_specs=(
            P(None, ("z", "y"), ("x", "c")),
            P(None, ("z", "y"), ("x", "c")),
            P(None, over),
            P(None, over),
        ),
        check_vma=False,
    )
```

```python
import math

import jax
import jax.numpy as jnp
from jax import lax
from jax.experimental import pallas as pl
from jax.experimental.pallas import tpu as pltpu
from jax.sharding import Mesh
from jax.sharding import PartitionSpec as P

D = 4096
FF = 10240
STEP = 4
M = 4
ROWS = 32
COLS = 1280
AXES = ("z", "y", "x", "c")
MESH = pl.DeviceIdType.MESH
HIGHEST = lax.Precision.HIGHEST
DECAY = 1.0 - float(STEP) ** (-0.8)
RATE = min(0.01, 1.0 / math.sqrt(STEP))
EPS = 1e-30
F32 = jnp.float32
TOP = 32767.0
PIECE = 3
PARTS = [(0, 0, 32), (1, 0, 32), (2, 0, 16), (2, 16, 16), (3, 0, 32)]
FIRST = 3

COL_PEERS = [(1, 0), (3, 0), (2, 0), (1, 1), (3, 1), (2, 1), (0, 1)]
LINE_PEERS = [1, 2, 3]


def iota(shape, dim):
    return lax.broadcasted_iota(jnp.int32, shape, dim)


def decoded(codes, steps, t, m):
    step = jnp.concatenate([steps[t, m : m + 1, :]] * (COLS // 256), axis=1)
    return codes[t, m].astype(jnp.int32).astype(F32) * step


def exchange_kernel(
    params, grads, row_hbm, col_hbm, map_hbm,
    new_out, change_out, p_out, s_out, rows_out, cols_out,
    g_in, by_row, by_col, gv, pv, qv, sv, row_old, col_old, old_map, stored, row_tiles, red_y, red_z, two_y, two_z, sc_x, sel, rnew,
    load_sem, small_sem, own_sem,
    s_tile, r_tile, s_line, r_line, s_grad, r_grad, s_par, r_par,
    s_row, r_row, s_red, r_red, s_sc, r_sc, s_col, r_col,
):
    z, y, x, c = (lax.axis_index(a) for a in AXES)
    k = x * 2 + c
    f = (z * 4 + y) * 8 + k

    def col_peer(i):
        dx, dc = COL_PEERS[i]
        return lax.rem(x + dx, 4), lax.rem(c + dc, 2)

    def to_cols(i, src, dst, ss, rs):
        tx, tc = col_peer(i)
        return pltpu.make_async_remote_copy(
            src_ref=src, dst_ref=dst, send_sem=ss, recv_sem=rs,
            device_id={"x": tx, "c": tc}, device_id_type=MESH,
        )

    def to_line(axis, d, src, dst, ss, rs):
        at = lax.rem((y if axis == "y" else z) + d, 4)
        return pltpu.make_async_remote_copy(
            src_ref=src, dst_ref=dst, send_sem=ss, recv_sem=rs,
            device_id={axis: at}, device_id_type=MESH,
        )

    def begin(copies):
        for cp in copies:
            cp.start()
        return copies

    def arrive(copies):
        for cp in copies:
            cp.wait_recv()

    barrier = pltpu.get_barrier_semaphore()
    for i in range(7):
        tx, tc = col_peer(i)
        pl.semaphore_signal(barrier, inc=1, device_id={"x": tx, "c": tc}, device_id_type=MESH)
    for d in LINE_PEERS:
        pl.semaphore_signal(barrier, inc=1, device_id={"y": lax.rem(y + d, 4)}, device_id_type=MESH)
        pl.semaphore_signal(barrier, inc=1, device_id={"z": lax.rem(z + d, 4)}, device_id_type=MESH)

    small = [
        pltpu.make_async_copy(row_hbm, row_old, small_sem.at[0]),
        pltpu.make_async_copy(col_hbm, col_old, small_sem.at[1]),
        pltpu.make_async_copy(map_hbm, old_map, small_sem.at[2]),
    ]
    begin(small)
    loads = []
    for m in range(M):
        loads.append(pltpu.make_async_copy(grads.at[m], gv.at[m], load_sem.at[m]))
    for m in range(M):
        loads.append(pltpu.make_async_copy(params.at[m], pv.at[m], load_sem.at[M + m]))
    begin(loads)

    pl.semaphore_wait(barrier, 13)

    def columns(i):
        tx, tc = col_peer(i)
        return pl.ds(pl.multiple_of((tx * 2 + tc) * COLS, 128), COLS)

    def send_grads(first, count, n):
        part = pl.ds(first, count)
        copies = [
            to_cols(i, grads.at[part, :, columns(i)], g_in.at[k, part], s_grad.at[n, i], r_grad.at[n, i])
            for i in range(7)
        ]
        return begin(copies)

    grad_copies = send_grads(0, 1, 0)

    mine = stored.at[pl.ds(pl.multiple_of(f * 8, 8), 8)]
    mine[...] = jnp.zeros((8, 128), F32)
    for cp in small:
        cp.wait()
    mine[0:4, 0:80] = col_old[...]
    mine[4:8, 0:32] = row_old[...]

    tiles = begin([to_cols(i, mine, mine, s_tile.at[i], r_tile.at[i]) for i in range(7)])
    grad_copies += send_grads(1, M - 1, 1)
    sent = tiles + grad_copies

    def peer_block(i):
        tx, tc = col_peer(i)
        return tx * 2 + tc

    def send_params(n):
        m, first, count = PARTS[n]
        rows = pl.ds(first, count)
        copies = begin(
            [
                to_cols(i, qv.at[peer_block(i), m, rows], p_out.at[k, m, rows], s_par.at[n, i], r_par.at[n, i])
                for i in range(7)
            ]
        )
        sent.extend(copies)
        return copies

    par_copies = []
    own_columns = pl.ds(pl.multiple_of(k * COLS, 128), COLS)
    lane32 = iota((ROWS, 128), 1)
    row_sums = jnp.zeros((ROWS, 128), F32)
    own = []
    for m in range(M):
        loads[m].wait()

        def add_squares(t, acc, m=m):
            g = gv[m, :, pl.ds(pl.multiple_of(t * COLS, 128), COLS)].astype(F32)
            sq = g * g + EPS
            for u in range(COLS // 128):
                acc = acc + sq[:, u * 128 : (u + 1) * 128]
            return acc

        part = lax.fori_loop(0, 8, add_squares, jnp.zeros((ROWS, 128), F32))
        total = jnp.sum(part, axis=1, keepdims=True)
        row_sums = row_sums + jnp.where(lane32 == m, total, 0.0)
        own.append(pltpu.make_async_copy(gv.at[m, :, own_columns], g_in.at[k, m], own_sem.at[m]))
        own[-1].start()

    at8 = iota((8, 128), 0)
    lane8 = iota((8, 128), 1)
    squares = jnp.zeros((8, 128), F32)
    for m in range(M):
        loads[M + m].wait()

        def add_weights(t, acc, m=m):
            w = pv[m, :, pl.ds(pl.multiple_of(t * COLS, 128), COLS)]
            sq = w * w
            tops = [jnp.zeros((8, 128), F32)] * 2
            size = jnp.abs(w)
            for u in range(COLS // 128):
                for v in range(ROWS // 8):
                    acc = acc + sq[v * 8 : (v + 1) * 8, u * 128 : (u + 1) * 128]
                    tops[u % 2] = jnp.maximum(tops[u % 2], size[v * 8 : (v + 1) * 8, u * 128 : (u + 1) * 128])
            top = jnp.concatenate([jnp.max(a, axis=0, keepdims=True) for a in tops], axis=1)
            top = jnp.maximum(top, 1e-30)
            sv[t, m : m + 1, :] = top * (1.0 / TOP)
            per = jnp.concatenate([TOP / top] * (COLS // 256), axis=1)
            qv[t, m] = jnp.round(w * per).astype(jnp.int32).astype(jnp.int16)
            return acc

        part = lax.fori_loop(0, 8, add_weights, jnp.zeros((8, 128), F32))
        total = jnp.sum(jnp.sum(part, axis=1, keepdims=True), axis=0, keepdims=True)
        squares = squares + jnp.where((at8 == m) & (lane8 == ROWS), total, 0.0)
        own.append(pltpu.make_async_copy(qv.at[k, m], p_out.at[k, m], own_sem.at[M + m]))
        own[-1].start()
    own.append(pltpu.make_async_copy(sv.at[k], s_out.at[k], own_sem.at[2 * M]))
    own[-1].start()
    steps = begin([to_cols(i, sv.at[peer_block(i)], s_out.at[k], s_par.at[len(PARTS), i], r_par.at[len(PARTS), i]) for i in range(7)])
    sent += steps

    arrive(tiles)
    line_at = stored.at[pl.ds(pl.multiple_of((z * 4 + y) * 64, 64), 64)]
    lines = begin([to_line("y", d, line_at, line_at, s_line.at[d - 1], r_line.at[d - 1]) for d in LINE_PEERS])
    sent += lines

    arrive(lines)
    slab_at = stored.at[pl.ds(pl.multiple_of(z * 256, 256), 256)]
    slabs = begin([to_line("z", d, slab_at, slab_at, s_line.at[d + 2], r_line.at[d + 2]) for d in LINE_PEERS])
    sent += slabs
    arrive(slabs)

    at_row = iota((128, 128), 0)
    picked = jnp.zeros((128, 128), F32)
    for m in range(M):
        onehot = jnp.where((at_row == m) & (old_map[m : m + 1, :] == f), 1.0, 0.0)
        picked = picked + jnp.dot(
            onehot, stored[pl.ds(4 + m, 128, stride=8), :], precision=HIGHEST, preferred_element_type=F32
        )
    sel[...] = jnp.zeros((128, COLS), F32)
    sel[0:ROWS, 0:128] = row_sums
    row_sums = jnp.transpose(sel[:, 0:128])[0:8, :]
    row_new = DECAY * picked[0:8, :] + (1.0 - DECAY) * row_sums / FF
    row_new = jnp.where((at8 < M) & (lane8 < ROWS), row_new, 1.0)
    own_tile = row_tiles.at[k]
    own_tile[...] = jnp.where(lane8 == ROWS, squares, row_new)[0:M, :]
    row_copies = begin([to_cols(i, own_tile, own_tile, s_row.at[i], r_row.at[i]) for i in range(7)])
    sent += row_copies
    for n in range(FIRST):
        par_copies.append(send_params(n))

    lane = iota((1, COLS), 1)
    block_of = ((lane.astype(F32) + 0.5) * (1.0 / 80.0)).astype(jnp.int32)
    place_of = lane - 80 * block_of
    at64 = iota((64, 128), 0)
    blocks = jnp.zeros((64, 128), F32)
    for m in range(M):
        wanted = (at64 - 16 * m) + k * 16
        inside = (at64 >= 16 * m) & (at64 < 16 * m + 16)
        onehot = jnp.where(inside & (old_map[m : m + 1, :] == wanted), 1.0, 0.0)
        blocks = blocks + jnp.dot(
            onehot, stored[pl.ds(m, 128, stride=8), :], precision=HIGHEST, preferred_element_type=F32
        )
    sel[0:64, 0:128] = blocks
    spread = jnp.where(iota((128, COLS), 0) == place_of, 1.0, 0.0)
    wide = jnp.dot(sel[0:64, 0:128], spread, precision=HIGHEST, preferred_element_type=F32)
    sel[0:64, :] = wide
    at16 = iota((16, COLS), 0)
    old_cols = [
        jnp.sum(jnp.where(at16 == block_of, sel[m * 16 : (m + 1) * 16, :], 0.0), axis=0, keepdims=True)
        for m in range(M)
    ]
    for m in range(M):
        by_col[m : m + 1, :] = old_cols[m]

    arrive(grad_copies)
    for m in range(M):
        own[m].wait()
    arrive(row_copies)
    tile_sum = row_tiles[0]
    for t in range(1, 8):
        tile_sum = tile_sum + row_tiles[t]
    lane4 = iota((M, 128), 1)
    row_sum = jnp.sum(jnp.where(lane4 < ROWS, tile_sum, 0.0), axis=1, keepdims=True)
    weight_sum = jnp.sum(jnp.where(lane4 == ROWS, tile_sum, 0.0), axis=1, keepdims=True)
    two_y[y] = jnp.where(lane4 == 0, row_sum, jnp.where(lane4 == 1, weight_sum, 0.0))
    own_row = z * 4 + y
    rows_out[own_row] = row_tiles[...]
    sel[:, 128:256] = jnp.ones((128, 128), F32)
    for t in range(8):
        sel[t * 8 : t * 8 + M, 128:256] = row_tiles[t]
    rnew[...] = 1.0 / jnp.transpose(sel[:, 128:256])[0:ROWS, :]

    for m in range(M):

        def add_columns(t, sums, m=m):
            plain, scaled = sums
            row = jnp.sum(jnp.where(lane32 == t * 8 + m, rnew[...], 0.0), axis=1, keepdims=True)
            g = g_in[t, m].astype(F32)
            sq = g * g
            by_rows = sq * row
            sq = sq + EPS
            for v in range(ROWS // 8):
                plain = plain + sq[v * 8 : (v + 1) * 8, :]
                scaled = scaled + by_rows[v * 8 : (v + 1) * 8, :]
            return plain, scaled

        nothing = jnp.zeros((8, COLS), F32)
        plain, scaled = lax.fori_loop(0, 8, add_columns, (nothing, nothing))
        red_y[y, m : m + 1, :] = jnp.sum(plain, axis=0, keepdims=True)
        red_y[y, M + m : M + m + 1, :] = jnp.sum(scaled, axis=0, keepdims=True)

    def reduce_over(axis, at, big, little, n):
        copies = []
        for d in LINE_PEERS:
            copies.append(to_line(axis, d, little.at[at], little.at[at], s_red.at[n + d - 1], r_red.at[n + d - 1]))
            copies.append(to_line(axis, d, big.at[at], big.at[at], s_red.at[n + d + 2], r_red.at[n + d + 2]))
        return begin(copies)

    stage = reduce_over("y", y, red_y, two_y, 0)
    own_rows = rows_out.at[pl.ds(own_row, 1)]
    rows_y = begin(
        [to_line("y", d, own_rows, own_rows, s_red.at[d + 11], r_red.at[d + 11]) for d in LINE_PEERS]
    )
    arrive(stage)
    sent += stage + rows_y
    red_z[z] = red_y[0] + red_y[1] + red_y[2] + red_y[3]
    two_z[z] = two_y[0] + two_y[1] + two_y[2] + two_y[3]
    stage = reduce_over("z", z, red_z, two_z, 6)
    arrive(rows_y)
    slab_rows = rows_out.at[pl.ds(pl.multiple_of(z * 4, 4), 4)]
    rows_z = begin(
        [to_line("z", d, slab_rows, slab_rows, s_red.at[d + 14], r_red.at[d + 14]) for d in LINE_PEERS]
    )
    arrive(stage)
    sent += stage + rows_z
    total = red_z[0] + red_z[1] + red_z[2] + red_z[3]
    two = two_z[0] + two_z[1] + two_z[2] + two_z[3]

    row_mean = two[:, 0:1] / D
    param_scale = jnp.sqrt(two[:, 1:2] / (D * FF) + 1e-6)
    col_new = DECAY * by_col[0:M, :] + (1.0 - DECAY) * total[0:M, :] / D
    sel[0:M, :] = col_new
    piece = lax.min(y * PIECE, COLS // 128 - PIECE)
    cols_out[y, k] = sel[0:M, pl.ds(pl.multiple_of(piece * 128, 128), PIECE * 128)]
    inv_col = 1.0 / col_new

    update_sum = jnp.sum(total[M : 2 * M, :] * inv_col, axis=1, keepdims=True) * row_mean
    sc_x[k] = jnp.broadcast_to(jnp.sum(update_sum, axis=0, keepdims=True), (M, 128))
    sums = begin([to_cols(i, sc_x.at[k], sc_x.at[k], s_sc.at[i], r_sc.at[i]) for i in range(7)])
    own_col = cols_out.at[y, k]
    cols_x = begin([to_cols(i, own_col, own_col, s_col.at[i], r_col.at[i]) for i in range(7)])
    sent += sums + cols_x

    for n in range(FIRST, len(PARTS)):
        par_copies.append(send_params(n))

    arrive(sums)
    update_sum = sc_x[0]
    for t in range(1, 8):
        update_sum = update_sum + sc_x[t]
    arrive(cols_x)
    own_cols = cols_out.at[pl.ds(y, 1)]
    cols_y = begin(
        [to_line("y", d, own_cols, own_cols, s_col.at[d + 6], r_col.at[d + 6]) for d in LINE_PEERS]
    )
    sent += cols_y
    update_total = update_sum[0:1, 0:1]
    clip = jnp.maximum(1.0, jnp.sqrt(update_total / (M * D * FF)))
    factors = -(RATE * param_scale) / clip * jnp.sqrt(row_mean)
    factor = jnp.zeros((1, 128), F32)
    for m in range(M):
        own_factor = factors[m : m + 1, :]
        factor = factor + jnp.where(lax.rem(iota((1, 128), 1), 8) == m, own_factor, 0.0)
    by_row[...] = factor * jnp.sqrt(rnew[...])
    by_col[0:M, :] = jnp.sqrt(inv_col)

    def block_of_rows(t):
        return pl.ds(pl.multiple_of(t * ROWS, ROWS), ROWS)

    for m in range(M):
        col = by_col[m : m + 1, :]

        def put_change(t, carry, m=m, col=col):
            row = jnp.sum(jnp.where(lane32 == t * 8 + m, by_row[...], 0.0), axis=1, keepdims=True)
            change_out[m, block_of_rows(t), :] = (g_in[t, m].astype(F32) * row) * col
            return carry

        lax.fori_loop(0, 8, put_change, 0)
    arrive(steps)
    own[2 * M].wait()
    arrive(rows_z)
    arrive(cols_y)
    for m in range(M):
        for n, part in enumerate(PARTS):
            if part[0] == m:
                arrive(par_copies[n])
        own[M + m].wait()
        if m == M - 1:
            break

        def put_weights(t, carry, m=m):
            new_out[m, block_of_rows(t), :] = decoded(p_out, s_out, t, m) + change_out[m, block_of_rows(t), :]
            return carry

        lax.fori_loop(0, 8, put_weights, 0)
    for cp in sent:
        cp.wait_send()


def apply_kernel(
    new_ref, change_ref, p_ref, s_ref, rows_ref, cols_ref, map_hbm,
    new_hbm, change_hbm, row_hbm, col_hbm,
    last_buf, row_buf, col_buf, new_map, big_sem, last_sem, small_sem,
):
    fetch = pltpu.make_async_copy(map_hbm, new_map, small_sem.at[0])
    fetch.start()
    big = [pltpu.make_async_copy(change_ref.at[m], change_hbm.at[m], big_sem.at[0, m]) for m in range(M)]
    big += [pltpu.make_async_copy(new_ref.at[m], new_hbm.at[m], big_sem.at[1, m]) for m in range(M - 1)]
    for cp in big:
        cp.start()

    last = []
    for t in range(8):
        rows = pl.ds(t * ROWS, ROWS)
        last_buf[rows, :] = decoded(p_ref, s_ref, t, M - 1) + change_ref[M - 1, rows, :]
        last.append(pltpu.make_async_copy(last_buf.at[rows], new_hbm.at[M - 1, rows], last_sem.at[t]))
        last[-1].start()

    fetch.wait()
    f = lax.axis_index(AXES)
    for n in range(M):
        b = new_map[n, f]
        row_buf[n : n + 1, :] = rows_ref[b // 8, lax.rem(b, 8), n : n + 1, 0:32]
        start = lax.rem(b, 16) * 80
        first = start // 128
        pair = []
        for t in (first, lax.min(first + 1, COLS // 128 - 1)):
            piece = lax.min(t // PIECE, 3)
            at = t - lax.min(piece * PIECE, COLS // 128 - PIECE)
            pair.append(cols_ref[piece, b // 16, n : n + 1, pl.ds(pl.multiple_of(at * 128, 128), 128)])
        pair = jnp.broadcast_to(jnp.concatenate(pair, axis=1), (8, 256))
        take = jnp.where(iota((256, 128), 0) == start - first * 128 + iota((256, 128), 1), 1.0, 0.0)
        got = jnp.dot(pair, take, precision=HIGHEST, preferred_element_type=F32)
        col_buf[n : n + 1, :] = got[0:1, 0:80]
    small = [
        pltpu.make_async_copy(row_buf, row_hbm, small_sem.at[1]),
        pltpu.make_async_copy(col_buf, col_hbm, small_sem.at[2]),
    ]
    for cp in small:
        cp.start()

    for cp in big + last + small:
        cp.wait()


def shards(params, grads, row_state_old, col_state_old, old_map, new_map):
    vmem = pl.BlockSpec(memory_space=pltpu.VMEM)
    hbm = pl.BlockSpec(memory_space=pltpu.HBM)
    dma = pltpu.SemaphoreType.DMA
    given = (params, grads, row_state_old, col_state_old, old_map)
    held = [pltpu.with_memory_space_constraint(a, pltpu.HBM) for a in given]
    held_map = pltpu.with_memory_space_constraint(new_map, pltpu.HBM)
    moved = pl.pallas_call(
        exchange_kernel,
        out_shape=[
            pltpu.VMEM((M - 1, 256, COLS), F32),
            pltpu.VMEM((M, 256, COLS), F32),
            pltpu.VMEM((8, M, ROWS, COLS), jnp.int16),
            pltpu.VMEM((8, M, 256), F32),
            pltpu.VMEM((16, 8, M, 128), F32),
            pltpu.VMEM((4, 8, M, PIECE * 128), F32),
        ],
        in_specs=[hbm] * 5,
        out_specs=[vmem] * 6,
        scratch_shapes=[
            pltpu.VMEM((8, M, ROWS, COLS), jnp.bfloat16),
            pltpu.VMEM((ROWS, 128), F32),
            pltpu.VMEM((8, COLS), F32),
            pltpu.VMEM((M, ROWS, FF), jnp.bfloat16),
            pltpu.VMEM((M, ROWS, FF), F32),
            pltpu.VMEM((8, M, ROWS, COLS), jnp.int16),
            pltpu.VMEM((8, M, 256), F32),
            pltpu.VMEM((M, 32), F32),
            pltpu.VMEM((M, 80), F32),
            pltpu.VMEM((M, 128), jnp.int32),
            pltpu.VMEM((1024, 128), F32),
            pltpu.VMEM((8, M, 128), F32),
            pltpu.VMEM((4, 8, COLS), F32),
            pltpu.VMEM((4, 8, COLS), F32),
            pltpu.VMEM((4, M, 128), F32),
            pltpu.VMEM((4, M, 128), F32),
            pltpu.VMEM((8, M, 128), F32),
            pltpu.VMEM((128, COLS), F32),
            pltpu.VMEM((ROWS, 128), F32),
            dma((2 * M,)),
            dma((3,)),
            dma((2 * M + 1,)),
            dma((7,)), dma((7,)),
            dma((6,)), dma((6,)),
            dma((2, 7)), dma((2, 7)),
            dma((len(PARTS) + 1, 7)), dma((len(PARTS) + 1, 7)),
            dma((7,)), dma((7,)),
            dma((18,)), dma((18,)),
            dma((7,)), dma((7,)),
            dma((10,)), dma((10,)),
        ],
        compiler_params=pltpu.CompilerParams(
            collective_id=0, has_side_effects=True, vmem_limit_bytes=28 << 20
        ),
        name="exchange",
    )(*held)
    return pl.pallas_call(
        apply_kernel,
        out_shape=[
            jax.ShapeDtypeStruct((M, 256, COLS), F32),
            jax.ShapeDtypeStruct((M, 256, COLS), F32),
            jax.ShapeDtypeStruct((M, 32), F32),
            jax.ShapeDtypeStruct((M, 80), F32),
        ],
        in_specs=[vmem] * 6 + [hbm],
        out_specs=[hbm] * 4,
        scratch_shapes=[
            pltpu.VMEM((256, COLS), F32),
            pltpu.VMEM((M, 32), F32),
            pltpu.VMEM((M, 80), F32),
            pltpu.SMEM((M, 128), jnp.int32),
            dma((2, M)),
            dma((8,)),
            dma((3,)),
        ],
        compiler_params=pltpu.CompilerParams(vmem_limit_bytes=28 << 20),
        name="apply",
    )(*(pltpu.with_memory_space_constraint(a, pltpu.VMEM) for a in moved), held_map)


def solution(mesh):
    torus = Mesh(mesh.devices.reshape(4, 4, 4, 2), AXES)
    over = ("z", "y", "x", "c")
    return jax.shard_map(
        shards,
        mesh=torus,
        in_specs=(P(None, over, None), P(None, over, None), P(None, over), P(None, over), P(), P()),
        out_specs=(
            P(None, ("z", "y"), ("x", "c")),
            P(None, ("z", "y"), ("x", "c")),
            P(None, over),
            P(None, over),
        ),
        check_vma=False,
    )
```

```python
import math

import jax
import jax.numpy as jnp
from jax import lax
from jax.experimental import pallas as pl
from jax.experimental.pallas import tpu as pltpu
from jax.sharding import Mesh
from jax.sharding import PartitionSpec as P

D = 4096
FF = 10240
STEP = 4
M = 4
ROWS = 32
COLS = 1280
AXES = ("z", "y", "x", "c")
MESH = pl.DeviceIdType.MESH
HIGHEST = lax.Precision.HIGHEST
DECAY = 1.0 - float(STEP) ** (-0.8)
RATE = min(0.01, 1.0 / math.sqrt(STEP))
EPS = 1e-30
F32 = jnp.float32
TOP = 32767.0
PIECE = 3
PARTS = [(0, 0, 32), (1, 0, 32), (2, 0, 16), (2, 16, 16), (3, 0, 32)]
FIRST = 3
LEADER = 4

COL_PEERS = [(1, 0), (3, 0), (2, 0), (1, 1), (3, 1), (2, 1), (0, 1)]
LINE_PEERS = [1, 2, 3]


def iota(shape, dim):
    return lax.broadcasted_iota(jnp.int32, shape, dim)


def decoded(codes, steps, t, m):
    step = jnp.concatenate([steps[t, m : m + 1, :]] * (COLS // 256), axis=1)
    return codes[t, m].astype(jnp.int32).astype(F32) * step


def exchange_kernel(
    params, grads, row_hbm, col_hbm, map_hbm,
    new_out, change_out, p_out, s_out, rows_out, cols_out,
    g_in, by_row, by_col, gv, pv, qv, sv, row_old, col_old, old_map, stored, row_tiles, red_y, red_z, two_y, two_z, sc_x, sel, rnew,
    lead_sem, go_sem, load_sem, small_sem, own_sem,
    s_tile, r_tile, s_line, r_line, s_grad, r_grad, s_par, r_par,
    s_row, r_row, s_red, r_red, s_sc, r_sc, s_col, r_col,
):
    z, y, x, c = (lax.axis_index(a) for a in AXES)
    k = x * 2 + c
    f = (z * 4 + y) * 8 + k

    def col_peer(i):
        dx, dc = COL_PEERS[i]
        return lax.rem(x + dx, 4), lax.rem(c + dc, 2)

    def to_cols(i, src, dst, ss, rs):
        tx, tc = col_peer(i)
        return pltpu.make_async_remote_copy(
            src_ref=src, dst_ref=dst, send_sem=ss, recv_sem=rs,
            device_id={"x": tx, "c": tc}, device_id_type=MESH,
        )

    def to_line(axis, d, src, dst, ss, rs):
        at = lax.rem((y if axis == "y" else z) + d, 4)
        return pltpu.make_async_remote_copy(
            src_ref=src, dst_ref=dst, send_sem=ss, recv_sem=rs,
            device_id={axis: at}, device_id_type=MESH,
        )

    def begin(copies):
        for cp in copies:
            cp.start()
        return copies

    def arrive(copies):
        for cp in copies:
            cp.wait_recv()

    barrier = pltpu.get_barrier_semaphore()
    for i in range(7):
        tx, tc = col_peer(i)
        pl.semaphore_signal(barrier, inc=1, device_id={"x": tx, "c": tc}, device_id_type=MESH)

    def signal_lines(sem):
        for d in LINE_PEERS:
            pl.semaphore_signal(sem, inc=1, device_id={"y": lax.rem(y + d, 4)}, device_id_type=MESH)
            pl.semaphore_signal(sem, inc=1, device_id={"z": lax.rem(z + d, 4)}, device_id_type=MESH)

    @pl.when(k == LEADER)
    def _():
        signal_lines(barrier)


    small = [
        pltpu.make_async_copy(row_hbm, row_old, small_sem.at[0]),
        pltpu.make_async_copy(col_hbm, col_old, small_sem.at[1]),
        pltpu.make_async_copy(map_hbm, old_map, small_sem.at[2]),
    ]
    loads = []
    for m in range(M):
        loads.append(pltpu.make_async_copy(grads.at[m], gv.at[m], load_sem.at[m]))
    for m in range(M):
        loads.append(pltpu.make_async_copy(params.at[m], pv.at[m], load_sem.at[M + m]))
    begin(loads[0:1] + small + loads[1:])

    @pl.when(k == LEADER)
    def _():
        pl.semaphore_wait(barrier, 13)

    @pl.when(k != LEADER)
    def _():
        pl.semaphore_wait(barrier, 7)


    def columns(i):
        tx, tc = col_peer(i)
        return pl.ds(pl.multiple_of((tx * 2 + tc) * COLS, 128), COLS)

    def send_grads(first, count, n):
        part = pl.ds(first, count)
        for m in range(first, first + count):
            loads[m].wait()
        copies = [
            to_cols(i, gv.at[part, :, columns(i)], g_in.at[k, part], s_grad.at[n, i], r_grad.at[n, i])
            for i in range(7)
        ]
        return begin(copies)

    grad_copies = send_grads(0, 1, 0)

    @pl.when(k == LEADER)
    def _():
        signal_lines(lead_sem)

    mine = stored.at[pl.ds(pl.multiple_of(f * 8, 8), 8)]
    mine[...] = jnp.zeros((8, 128), F32)
    for cp in small:
        cp.wait()
    mine[0:4, 0:80] = col_old[...]
    mine[4:8, 0:32] = row_old[...]

    tiles = begin([to_cols(i, mine, mine, s_tile.at[i], r_tile.at[i]) for i in range(7)])
    grad_copies += send_grads(1, M - 1, 1)
    sent = tiles + grad_copies

    def peer_block(i):
        tx, tc = col_peer(i)
        return tx * 2 + tc

    def send_params(n):
        m, first, count = PARTS[n]
        rows = pl.ds(first, count)
        copies = begin(
            [
                to_cols(i, qv.at[peer_block(i), m, rows], p_out.at[k, m, rows], s_par.at[n, i], r_par.at[n, i])
                for i in range(7)
            ]
        )
        sent.extend(copies)
        return copies

    par_copies = []
    own_columns = pl.ds(pl.multiple_of(k * COLS, 128), COLS)
    lane32 = iota((ROWS, 128), 1)
    row_sums = jnp.zeros((ROWS, 128), F32)
    own = []
    for m in range(M):

        def add_squares(t, acc, m=m):
            g = gv[m, :, pl.ds(pl.multiple_of(t * COLS, 128), COLS)].astype(F32)
            sq = g * g + EPS
            for u in range(COLS // 128):
                acc = acc + sq[:, u * 128 : (u + 1) * 128]
            return acc

        part = lax.fori_loop(0, 8, add_squares, jnp.zeros((ROWS, 128), F32))
        total = jnp.sum(part, axis=1, keepdims=True)
        row_sums = row_sums + jnp.where(lane32 == m, total, 0.0)
        own.append(pltpu.make_async_copy(gv.at[m, :, own_columns], g_in.at[k, m], own_sem.at[m]))
        own[-1].start()

    at8 = iota((8, 128), 0)
    lane8 = iota((8, 128), 1)
    squares = jnp.zeros((8, 128), F32)
    for m in range(M):
        loads[M + m].wait()

        def add_weights(t, acc, m=m):
            w = pv[m, :, pl.ds(pl.multiple_of(t * COLS, 128), COLS)]
            sq = w * w
            tops = [jnp.zeros((8, 128), F32)] * 2
            size = jnp.abs(w)
            for u in range(COLS // 128):
                for v in range(ROWS // 8):
                    acc = acc + sq[v * 8 : (v + 1) * 8, u * 128 : (u + 1) * 128]
                    tops[u % 2] = jnp.maximum(tops[u % 2], size[v * 8 : (v + 1) * 8, u * 128 : (u + 1) * 128])
            top = jnp.concatenate([jnp.max(a, axis=0, keepdims=True) for a in tops], axis=1)
            top = jnp.maximum(top, 1e-30)
            sv[t, m : m + 1, :] = top * (1.0 / TOP)
            per = jnp.concatenate([TOP / top] * (COLS // 256), axis=1)
            qv[t, m] = jnp.round(w * per).astype(jnp.int32).astype(jnp.int16)
            return acc

        part = lax.fori_loop(0, 8, add_weights, jnp.zeros((8, 128), F32))
        total = jnp.sum(jnp.sum(part, axis=1, keepdims=True), axis=0, keepdims=True)
        squares = squares + jnp.where((at8 == m) & (lane8 == ROWS), total, 0.0)
        own.append(pltpu.make_async_copy(qv.at[k, m], p_out.at[k, m], own_sem.at[M + m]))
        own[-1].start()
    own.append(pltpu.make_async_copy(sv.at[k], s_out.at[k], own_sem.at[2 * M]))
    own[-1].start()
    steps = begin([to_cols(i, sv.at[peer_block(i)], s_out.at[k], s_par.at[len(PARTS), i], r_par.at[len(PARTS), i]) for i in range(7)])
    sent += steps

    arrive(tiles)

    @pl.when(k == LEADER)
    def _():
        pl.semaphore_wait(lead_sem, 6)
        for i in range(7):
            tx, tc = col_peer(i)
            pl.semaphore_signal(go_sem, inc=1, device_id={"x": tx, "c": tc}, device_id_type=MESH)

    @pl.when(k != LEADER)
    def _():
        pl.semaphore_wait(go_sem, 1)

    line_at = stored.at[pl.ds(pl.multiple_of((z * 4 + y) * 64, 64), 64)]
    lines = begin([to_line("y", d, line_at, line_at, s_line.at[d - 1], r_line.at[d - 1]) for d in LINE_PEERS])
    sent += lines

    arrive(lines)
    slab_at = stored.at[pl.ds(pl.multiple_of(z * 256, 256), 256)]
    slabs = begin([to_line("z", d, slab_at, slab_at, s_line.at[d + 2], r_line.at[d + 2]) for d in LINE_PEERS])
    sent += slabs
    arrive(slabs)

    at_row = iota((128, 128), 0)
    picked = jnp.zeros((128, 128), F32)
    for m in range(M):
        onehot = jnp.where((at_row == m) & (old_map[m : m + 1, :] == f), 1.0, 0.0)
        picked = picked + jnp.dot(
            onehot, stored[pl.ds(4 + m, 128, stride=8), :], precision=HIGHEST, preferred_element_type=F32
        )
    sel[...] = jnp.zeros((128, COLS), F32)
    sel[0:ROWS, 0:128] = row_sums
    row_sums = jnp.transpose(sel[:, 0:128])[0:8, :]
    row_new = DECAY * picked[0:8, :] + (1.0 - DECAY) * row_sums / FF
    row_new = jnp.where((at8 < M) & (lane8 < ROWS), row_new, 1.0)
    own_tile = row_tiles.at[k]
    own_tile[...] = jnp.where(lane8 == ROWS, squares, row_new)[0:M, :]
    row_copies = begin([to_cols(i, own_tile, own_tile, s_row.at[i], r_row.at[i]) for i in range(7)])
    sent += row_copies
    for n in range(FIRST):
        par_copies.append(send_params(n))

    lane = iota((1, COLS), 1)
    block_of = ((lane.astype(F32) + 0.5) * (1.0 / 80.0)).astype(jnp.int32)
    place_of = lane - 80 * block_of
    at64 = iota((64, 128), 0)
    blocks = jnp.zeros((64, 128), F32)
    for m in range(M):
        wanted = (at64 - 16 * m) + k * 16
        inside = (at64 >= 16 * m) & (at64 < 16 * m + 16)
        onehot = jnp.where(inside & (old_map[m : m + 1, :] == wanted), 1.0, 0.0)
        blocks = blocks + jnp.dot(
            onehot, stored[pl.ds(m, 128, stride=8), :], precision=HIGHEST, preferred_element_type=F32
        )
    sel[0:64, 0:128] = blocks
    spread = jnp.where(iota((128, COLS), 0) == place_of, 1.0, 0.0)
    wide = jnp.dot(sel[0:64, 0:128], spread, precision=HIGHEST, preferred_element_type=F32)
    sel[0:64, :] = wide
    at16 = iota((16, COLS), 0)
    old_cols = [
        jnp.sum(jnp.where(at16 == block_of, sel[m * 16 : (m + 1) * 16, :], 0.0), axis=0, keepdims=True)
        for m in range(M)
    ]
    for m in range(M):
        by_col[m : m + 1, :] = old_cols[m]

    arrive(grad_copies)
    for m in range(M):
        own[m].wait()
    arrive(row_copies)
    tile_sum = row_tiles[0]
    for t in range(1, 8):
        tile_sum = tile_sum + row_tiles[t]
    lane4 = iota((M, 128), 1)
    row_sum = jnp.sum(jnp.where(lane4 < ROWS, tile_sum, 0.0), axis=1, keepdims=True)
    weight_sum = jnp.sum(jnp.where(lane4 == ROWS, tile_sum, 0.0), axis=1, keepdims=True)
    two_y[y] = jnp.where(lane4 == 0, row_sum, jnp.where(lane4 == 1, weight_sum, 0.0))
    own_row = z * 4 + y
    rows_out[own_row] = row_tiles[...]
    sel[:, 128:256] = jnp.ones((128, 128), F32)
    for t in range(8):
        sel[t * 8 : t * 8 + M, 128:256] = row_tiles[t]
    rnew[...] = 1.0 / jnp.transpose(sel[:, 128:256])[0:ROWS, :]

    for m in range(M):

        def add_columns(t, sums, m=m):
            plain, scaled = sums
            row = jnp.sum(jnp.where(lane32 == t * 8 + m, rnew[...], 0.0), axis=1, keepdims=True)
            g = g_in[t, m].astype(F32)
            sq = g * g
            by_rows = sq * row
            sq = sq + EPS
            for v in range(ROWS // 8):
                plain = plain + sq[v * 8 : (v + 1) * 8, :]
                scaled = scaled + by_rows[v * 8 : (v + 1) * 8, :]
            return plain, scaled

        nothing = jnp.zeros((8, COLS), F32)
        plain, scaled = lax.fori_loop(0, 8, add_columns, (nothing, nothing))
        red_y[y, m : m + 1, :] = jnp.sum(plain, axis=0, keepdims=True)
        red_y[y, M + m : M + m + 1, :] = jnp.sum(scaled, axis=0, keepdims=True)

    def reduce_over(axis, at, big, little, n):
        copies = []
        for d in LINE_PEERS:
            copies.append(to_line(axis, d, little.at[at], little.at[at], s_red.at[n + d - 1], r_red.at[n + d - 1]))
            copies.append(to_line(axis, d, big.at[at], big.at[at], s_red.at[n + d + 2], r_red.at[n + d + 2]))
        return begin(copies)

    stage = reduce_over("y", y, red_y, two_y, 0)
    own_rows = rows_out.at[pl.ds(own_row, 1)]
    rows_y = begin(
        [to_line("y", d, own_rows, own_rows, s_red.at[d + 11], r_red.at[d + 11]) for d in LINE_PEERS]
    )
    arrive(stage)
    sent += stage + rows_y
    red_z[z] = red_y[0] + red_y[1] + red_y[2] + red_y[3]
    two_z[z] = two_y[0] + two_y[1] + two_y[2] + two_y[3]
    stage = reduce_over("z", z, red_z, two_z, 6)
    arrive(rows_y)
    slab_rows = rows_out.at[pl.ds(pl.multiple_of(z * 4, 4), 4)]
    rows_z = begin(
        [to_line("z", d, slab_rows, slab_rows, s_red.at[d + 14], r_red.at[d + 14]) for d in LINE_PEERS]
    )
    arrive(stage)
    sent += stage + rows_z
    total = red_z[0] + red_z[1] + red_z[2] + red_z[3]
    two = two_z[0] + two_z[1] + two_z[2] + two_z[3]

    row_mean = two[:, 0:1] / D
    param_scale = jnp.sqrt(two[:, 1:2] / (D * FF) + 1e-6)
    col_new = DECAY * by_col[0:M, :] + (1.0 - DECAY) * total[0:M, :] / D
    sel[0:M, :] = col_new
    piece = lax.min(y * PIECE, COLS // 128 - PIECE)
    cols_out[y, k] = sel[0:M, pl.ds(pl.multiple_of(piece * 128, 128), PIECE * 128)]
    inv_col = 1.0 / col_new

    update_sum = jnp.sum(total[M : 2 * M, :] * inv_col, axis=1, keepdims=True) * row_mean
    sc_x[k] = jnp.broadcast_to(jnp.sum(update_sum, axis=0, keepdims=True), (M, 128))
    sums = begin([to_cols(i, sc_x.at[k], sc_x.at[k], s_sc.at[i], r_sc.at[i]) for i in range(7)])
    own_col = cols_out.at[y, k]
    cols_x = begin([to_cols(i, own_col, own_col, s_col.at[i], r_col.at[i]) for i in range(7)])
    sent += sums + cols_x

    for n in range(FIRST, len(PARTS)):
        par_copies.append(send_params(n))

    arrive(sums)
    update_sum = sc_x[0]
    for t in range(1, 8):
        update_sum = update_sum + sc_x[t]
    arrive(cols_x)
    own_cols = cols_out.at[pl.ds(y, 1)]
    cols_y = begin(
        [to_line("y", d, own_cols, own_cols, s_col.at[d + 6], r_col.at[d + 6]) for d in LINE_PEERS]
    )
    sent += cols_y
    update_total = update_sum[0:1, 0:1]
    clip = jnp.maximum(1.0, jnp.sqrt(update_total / (M * D * FF)))
    factors = -(RATE * param_scale) / clip * jnp.sqrt(row_mean)
    factor = jnp.zeros((1, 128), F32)
    for m in range(M):
        own_factor = factors[m : m + 1, :]
        factor = factor + jnp.where(lax.rem(iota((1, 128), 1), 8) == m, own_factor, 0.0)
    by_row[...] = factor * jnp.sqrt(rnew[...])
    by_col[0:M, :] = jnp.sqrt(inv_col)

    def block_of_rows(t):
        return pl.ds(pl.multiple_of(t * ROWS, ROWS), ROWS)

    for m in range(M):
        col = by_col[m : m + 1, :]

        def put_change(t, carry, m=m, col=col):
            row = jnp.sum(jnp.where(lane32 == t * 8 + m, by_row[...], 0.0), axis=1, keepdims=True)
            change_out[m, block_of_rows(t), :] = (g_in[t, m].astype(F32) * row) * col
            return carry

        lax.fori_loop(0, 8, put_change, 0)
    arrive(steps)
    own[2 * M].wait()
    arrive(rows_z)
    arrive(cols_y)
    for m in range(M):
        for n, part in enumerate(PARTS):
            if part[0] == m:
                arrive(par_copies[n])
        own[M + m].wait()
        if m == M - 1:
            break

        def put_weights(t, carry, m=m):
            new_out[m, block_of_rows(t), :] = decoded(p_out, s_out, t, m) + change_out[m, block_of_rows(t), :]
            return carry

        lax.fori_loop(0, 8, put_weights, 0)
    for cp in sent:
        cp.wait_send()


def apply_kernel(
    new_ref, change_ref, p_ref, s_ref, rows_ref, cols_ref, map_hbm,
    new_hbm, change_hbm, row_hbm, col_hbm,
    last_buf, row_buf, col_buf, new_map, big_sem, last_sem, small_sem,
):
    fetch = pltpu.make_async_copy(map_hbm, new_map, small_sem.at[0])
    fetch.start()
    big = [pltpu.make_async_copy(change_ref.at[m], change_hbm.at[m], big_sem.at[0, m]) for m in range(M)]
    big += [pltpu.make_async_copy(new_ref.at[m], new_hbm.at[m], big_sem.at[1, m]) for m in range(M - 1)]
    for cp in big:
        cp.start()

    last = []
    for t in range(8):
        rows = pl.ds(t * ROWS, ROWS)
        last_buf[rows, :] = decoded(p_ref, s_ref, t, M - 1) + change_ref[M - 1, rows, :]
        last.append(pltpu.make_async_copy(last_buf.at[rows], new_hbm.at[M - 1, rows], last_sem.at[t]))
        last[-1].start()

    fetch.wait()
    f = lax.axis_index(AXES)
    for n in range(M):
        b = new_map[n, f]
        row_buf[n : n + 1, :] = rows_ref[b // 8, lax.rem(b, 8), n : n + 1, 0:32]
        start = lax.rem(b, 16) * 80
        first = start // 128
        pair = []
        for t in (first, lax.min(first + 1, COLS // 128 - 1)):
            piece = lax.min(t // PIECE, 3)
            at = t - lax.min(piece * PIECE, COLS // 128 - PIECE)
            pair.append(cols_ref[piece, b // 16, n : n + 1, pl.ds(pl.multiple_of(at * 128, 128), 128)])
        pair = jnp.broadcast_to(jnp.concatenate(pair, axis=1), (8, 256))
        take = jnp.where(iota((256, 128), 0) == start - first * 128 + iota((256, 128), 1), 1.0, 0.0)
        got = jnp.dot(pair, take, precision=HIGHEST, preferred_element_type=F32)
        col_buf[n : n + 1, :] = got[0:1, 0:80]
    small = [
        pltpu.make_async_copy(row_buf, row_hbm, small_sem.at[1]),
        pltpu.make_async_copy(col_buf, col_hbm, small_sem.at[2]),
    ]
    for cp in small:
        cp.start()

    for cp in big + last + small:
        cp.wait()


def shards(params, grads, row_state_old, col_state_old, old_map, new_map):
    vmem = pl.BlockSpec(memory_space=pltpu.VMEM)
    hbm = pl.BlockSpec(memory_space=pltpu.HBM)
    dma = pltpu.SemaphoreType.DMA
    given = (params, grads, row_state_old, col_state_old, old_map)
    held = [pltpu.with_memory_space_constraint(a, pltpu.HBM) for a in given]
    held_map = pltpu.with_memory_space_constraint(new_map, pltpu.HBM)
    moved = pl.pallas_call(
        exchange_kernel,
        out_shape=[
            pltpu.VMEM((M - 1, 256, COLS), F32),
            pltpu.VMEM((M, 256, COLS), F32),
            pltpu.VMEM((8, M, ROWS, COLS), jnp.int16),
            pltpu.VMEM((8, M, 256), F32),
            pltpu.VMEM((16, 8, M, 128), F32),
            pltpu.VMEM((4, 8, M, PIECE * 128), F32),
        ],
        in_specs=[hbm] * 5,
        out_specs=[vmem] * 6,
        scratch_shapes=[
            pltpu.VMEM((8, M, ROWS, COLS), jnp.bfloat16),
            pltpu.VMEM((ROWS, 128), F32),
            pltpu.VMEM((8, COLS), F32),
            pltpu.VMEM((M, ROWS, FF), jnp.bfloat16),
            pltpu.VMEM((M, ROWS, FF), F32),
            pltpu.VMEM((8, M, ROWS, COLS), jnp.int16),
            pltpu.VMEM((8, M, 256), F32),
            pltpu.VMEM((M, 32), F32),
            pltpu.VMEM((M, 80), F32),
            pltpu.VMEM((M, 128), jnp.int32),
            pltpu.VMEM((1024, 128), F32),
            pltpu.VMEM((8, M, 128), F32),
            pltpu.VMEM((4, 8, COLS), F32),
            pltpu.VMEM((4, 8, COLS), F32),
            pltpu.VMEM((4, M, 128), F32),
            pltpu.VMEM((4, M, 128), F32),
            pltpu.VMEM((8, M, 128), F32),
            pltpu.VMEM((128, COLS), F32),
            pltpu.VMEM((ROWS, 128), F32),
            pltpu.SemaphoreType.REGULAR,
            pltpu.SemaphoreType.REGULAR,
            dma((2 * M,)),
            dma((3,)),
            dma((2 * M + 1,)),
            dma((7,)), dma((7,)),
            dma((6,)), dma((6,)),
            dma((2, 7)), dma((2, 7)),
            dma((len(PARTS) + 1, 7)), dma((len(PARTS) + 1, 7)),
            dma((7,)), dma((7,)),
            dma((18,)), dma((18,)),
            dma((7,)), dma((7,)),
            dma((10,)), dma((10,)),
        ],
        compiler_params=pltpu.CompilerParams(
            collective_id=0, has_side_effects=True, vmem_limit_bytes=28 << 20
        ),
        name="exchange",
    )(*held)
    return pl.pallas_call(
        apply_kernel,
        out_shape=[
            jax.ShapeDtypeStruct((M, 256, COLS), F32),
            jax.ShapeDtypeStruct((M, 256, COLS), F32),
            jax.ShapeDtypeStruct((M, 32), F32),
            jax.ShapeDtypeStruct((M, 80), F32),
        ],
        in_specs=[vmem] * 6 + [hbm],
        out_specs=[hbm] * 4,
        scratch_shapes=[
            pltpu.VMEM((256, COLS), F32),
            pltpu.VMEM((M, 32), F32),
            pltpu.VMEM((M, 80), F32),
            pltpu.SMEM((M, 128), jnp.int32),
            dma((2, M)),
            dma((8,)),
            dma((3,)),
        ],
        compiler_params=pltpu.CompilerParams(vmem_limit_bytes=28 << 20),
        name="apply",
    )(*(pltpu.with_memory_space_constraint(a, pltpu.VMEM) for a in moved), held_map)


def solution(mesh):
    torus = Mesh(mesh.devices.reshape(4, 4, 4, 2), AXES)
    over = ("z", "y", "x", "c")
    return jax.shard_map(
        shards,
        mesh=torus,
        in_specs=(P(None, over, None), P(None, over, None), P(None, over), P(None, over), P(), P()),
        out_specs=(
            P(None, ("z", "y"), ("x", "c")),
            P(None, ("z", "y"), ("x", "c")),
            P(None, over),
            P(None, over),
        ),
        check_vma=False,
    )
```

```python
import math

import jax
import jax.numpy as jnp
from jax import lax
from jax.experimental import pallas as pl
from jax.experimental.pallas import tpu as pltpu
from jax.sharding import Mesh
from jax.sharding import PartitionSpec as P

D = 4096
FF = 10240
STEP = 4
M = 4
ROWS = 32
COLS = 1280
AXES = ("z", "y", "x", "c")
MESH = pl.DeviceIdType.MESH
HIGHEST = lax.Precision.HIGHEST
DECAY = 1.0 - float(STEP) ** (-0.8)
RATE = min(0.01, 1.0 / math.sqrt(STEP))
EPS = 1e-30
F32 = jnp.float32
TOP = 32767.0
PIECE = 3
PARTS = [(0, 0, 32), (1, 0, 32), (2, 0, 16), (2, 16, 16), (3, 0, 32)]
FIRST = 3
LEADER = 4

COL_PEERS = [(1, 0), (3, 0), (1, 1), (3, 1), (0, 1), (2, 0), (2, 1)]
NEAR = 5
ORDER = (0, 1, 5, 2, 3, 6, 4)
LINE_PEERS = [1, 2, 3]


def iota(shape, dim):
    return lax.broadcasted_iota(jnp.int32, shape, dim)


def decoded(codes, steps, t, m):
    step = jnp.concatenate([steps[t, m : m + 1, 0:256]] * (COLS // 256), axis=1)
    return codes[t, m].astype(jnp.int32).astype(F32) * step


def exchange_kernel(
    params, grads, row_hbm, col_hbm, map_hbm,
    new_out, change_out, p_out, s_out, rows_out, cols_out,
    g_in, by_row, by_col, gv, pv, qv, sv, row_old, col_old, old_map, stored, red_y, red_z, two_y, two_z, sel, rnew,
    far_sem, lead_sem, go_sem, load_sem, small_sem, own_sem,
    s_tile, r_tile, s_line, r_line, s_grad, r_grad, s_par, r_par,
    s_row, r_row, s_red, r_red, s_col, r_col,
):
    z, y, x, c = (lax.axis_index(a) for a in AXES)
    k = x * 2 + c
    f = (z * 4 + y) * 8 + k

    def col_peer(i):
        dx, dc = COL_PEERS[i]
        return lax.rem(x + dx, 4), lax.rem(c + dc, 2)

    def to_cols(i, src, dst, ss, rs):
        tx, tc = col_peer(i)
        return pltpu.make_async_remote_copy(
            src_ref=src, dst_ref=dst, send_sem=ss, recv_sem=rs,
            device_id={"x": tx, "c": tc}, device_id_type=MESH,
        )

    def to_line(axis, d, src, dst, ss, rs):
        at = lax.rem((y if axis == "y" else z) + d, 4)
        return pltpu.make_async_remote_copy(
            src_ref=src, dst_ref=dst, send_sem=ss, recv_sem=rs,
            device_id={axis: at}, device_id_type=MESH,
        )

    def begin(copies):
        for cp in copies:
            cp.start()
        return copies

    def arrive(copies):
        for cp in copies:
            cp.wait_recv()

    barrier = pltpu.get_barrier_semaphore()
    for i in range(NEAR):
        tx, tc = col_peer(i)
        pl.semaphore_signal(barrier, inc=1, device_id={"x": tx, "c": tc}, device_id_type=MESH)

    def signal_lines(sem):
        for d in LINE_PEERS:
            pl.semaphore_signal(sem, inc=1, device_id={"y": lax.rem(y + d, 4)}, device_id_type=MESH)
            pl.semaphore_signal(sem, inc=1, device_id={"z": lax.rem(z + d, 4)}, device_id_type=MESH)

    @pl.when(k == LEADER)
    def _():
        signal_lines(barrier)


    small = [
        pltpu.make_async_copy(row_hbm, row_old, small_sem.at[0]),
        pltpu.make_async_copy(col_hbm, col_old, small_sem.at[1]),
        pltpu.make_async_copy(map_hbm, old_map, small_sem.at[2]),
    ]
    loads = []
    for m in range(M):
        loads.append(pltpu.make_async_copy(grads.at[m], gv.at[m], load_sem.at[m]))
    for m in range(M):
        loads.append(pltpu.make_async_copy(params.at[m], pv.at[m], load_sem.at[M + m]))
    begin(loads[0:1] + small + loads[1:])

    @pl.when(k == LEADER)
    def _():
        pl.semaphore_wait(barrier, NEAR + 6)

    @pl.when(k != LEADER)
    def _():
        pl.semaphore_wait(barrier, NEAR)


    def columns(i):
        tx, tc = col_peer(i)
        return pl.ds(pl.multiple_of((tx * 2 + tc) * COLS, 128), COLS)

    def send_grads(first, count, n, peers):
        part = pl.ds(first, count)
        copies = [
            to_cols(i, gv.at[part, :, columns(i)], g_in.at[k, part], s_grad.at[n, i], r_grad.at[n, i])
            for i in peers
        ]
        return begin(copies)

    pl.semaphore_signal(far_sem, inc=1, device_id={"x": lax.rem(x + 3, 4)}, device_id_type=MESH)
    loads[0].wait()
    grad_copies = send_grads(0, 1, 0, range(NEAR))
    pl.semaphore_wait(far_sem, 1)
    grad_copies += send_grads(0, 1, 0, range(NEAR, 7))

    @pl.when(k == LEADER)
    def _():
        signal_lines(lead_sem)

    mine = stored.at[pl.ds(pl.multiple_of(f * 8, 8), 8)]
    mine[...] = jnp.zeros((8, 128), F32)
    for cp in small:
        cp.wait()
    mine[0:4, 0:80] = col_old[...]
    mine[4:8, 0:32] = row_old[...]

    tiles = begin([to_cols(i, mine, mine, s_tile.at[i], r_tile.at[i]) for i in range(7)])
    for m in range(1, M):
        loads[m].wait()
    grad_copies += send_grads(1, M - 1, 1, ORDER)
    sent = tiles + grad_copies

    def peer_block(i):
        tx, tc = col_peer(i)
        return tx * 2 + tc

    def send_params(n):
        m, first, count = PARTS[n]
        rows = pl.ds(first, count)
        copies = begin(
            [
                to_cols(i, qv.at[peer_block(i), m, rows], p_out.at[k, m, rows], s_par.at[n, i], r_par.at[n, i])
                for i in ORDER
            ]
        )
        sent.extend(copies)
        return copies

    par_copies = []
    own_columns = pl.ds(pl.multiple_of(k * COLS, 128), COLS)
    lane32 = iota((ROWS, 128), 1)
    row_sums = jnp.zeros((ROWS, 128), F32)
    own = []
    for m in range(M):

        def add_squares(t, acc, m=m):
            g = gv[m, :, pl.ds(pl.multiple_of(t * COLS, 128), COLS)].astype(F32)
            sq = g * g + EPS
            for u in range(COLS // 128):
                acc = acc + sq[:, u * 128 : (u + 1) * 128]
            return acc

        part = lax.fori_loop(0, 8, add_squares, jnp.zeros((ROWS, 128), F32))
        total = jnp.sum(part, axis=1, keepdims=True)
        row_sums = row_sums + jnp.where(lane32 == m, total, 0.0)
        own.append(pltpu.make_async_copy(gv.at[m, :, own_columns], g_in.at[k, m], own_sem.at[m]))
        own[-1].start()

    at8 = iota((8, 128), 0)
    lane8 = iota((8, 128), 1)
    squares = jnp.zeros((8, 128), F32)
    for m in range(M):
        loads[M + m].wait()

        def add_weights(t, acc, m=m):
            w = pv[m, :, pl.ds(pl.multiple_of(t * COLS, 128), COLS)]
            sq = w * w
            tops = [jnp.zeros((8, 128), F32)] * 2
            size = jnp.abs(w)
            for u in range(COLS // 128):
                for v in range(ROWS // 8):
                    acc = acc + sq[v * 8 : (v + 1) * 8, u * 128 : (u + 1) * 128]
                    tops[u % 2] = jnp.maximum(tops[u % 2], size[v * 8 : (v + 1) * 8, u * 128 : (u + 1) * 128])
            top = jnp.concatenate([jnp.max(a, axis=0, keepdims=True) for a in tops], axis=1)
            top = jnp.maximum(top, 1e-30)
            sv[t, m : m + 1, 0:256] = top * (1.0 / TOP)
            per = jnp.concatenate([TOP / top] * (COLS // 256), axis=1)
            qv[t, m] = jnp.round(w * per).astype(jnp.int32).astype(jnp.int16)
            return acc

        part = lax.fori_loop(0, 8, add_weights, jnp.zeros((8, 128), F32))
        total = jnp.sum(jnp.sum(part, axis=1, keepdims=True), axis=0, keepdims=True)
        squares = squares + jnp.where((at8 == m) & (lane8 == ROWS), total, 0.0)
        own.append(pltpu.make_async_copy(qv.at[k, m], p_out.at[k, m], own_sem.at[M + m]))
        own[-1].start()

    arrive(tiles)

    @pl.when(k == LEADER)
    def _():
        pl.semaphore_wait(lead_sem, 6)
        for i in range(7):
            tx, tc = col_peer(i)
            pl.semaphore_signal(go_sem, inc=1, device_id={"x": tx, "c": tc}, device_id_type=MESH)

    @pl.when(k != LEADER)
    def _():
        pl.semaphore_wait(go_sem, 1)

    line_at = stored.at[pl.ds(pl.multiple_of((z * 4 + y) * 64, 64), 64)]
    lines = begin([to_line("y", d, line_at, line_at, s_line.at[d - 1], r_line.at[d - 1]) for d in LINE_PEERS])
    sent += lines

    arrive(lines)
    slab_at = stored.at[pl.ds(pl.multiple_of(z * 256, 256), 256)]
    slabs = begin([to_line("z", d, slab_at, slab_at, s_line.at[d + 2], r_line.at[d + 2]) for d in LINE_PEERS])
    sent += slabs
    arrive(slabs)

    at_row = iota((128, 128), 0)
    picked = jnp.zeros((128, 128), F32)
    for m in range(M):
        onehot = jnp.where((at_row == m) & (old_map[m : m + 1, :] == f), 1.0, 0.0)
        picked = picked + jnp.dot(
            onehot, stored[pl.ds(4 + m, 128, stride=8), :], precision=HIGHEST, preferred_element_type=F32
        )
    sel[...] = jnp.zeros((128, COLS), F32)
    sel[0:ROWS, 0:128] = row_sums
    row_sums = jnp.transpose(sel[:, 0:128])[0:8, :]
    row_new = DECAY * picked[0:8, :] + (1.0 - DECAY) * row_sums / FF
    row_new = jnp.where((at8 < M) & (lane8 < ROWS), row_new, 1.0)
    own_tile = jnp.where(lane8 == ROWS, squares, row_new)[0:M, :]
    for t in range(8):
        sv[t, :, 256:384] = own_tile
    s_out[k] = sv[k]
    row_copies = begin([to_cols(i, sv.at[peer_block(i)], s_out.at[k], s_row.at[i], r_row.at[i]) for i in range(7)])
    sent += row_copies
    for n in range(FIRST):
        par_copies.append(send_params(n))

    lane = iota((1, COLS), 1)
    block_of = ((lane.astype(F32) + 0.5) * (1.0 / 80.0)).astype(jnp.int32)
    place_of = lane - 80 * block_of
    at64 = iota((64, 128), 0)
    blocks = jnp.zeros((64, 128), F32)
    for m in range(M):
        wanted = (at64 - 16 * m) + k * 16
        inside = (at64 >= 16 * m) & (at64 < 16 * m + 16)
        onehot = jnp.where(inside & (old_map[m : m + 1, :] == wanted), 1.0, 0.0)
        blocks = blocks + jnp.dot(
            onehot, stored[pl.ds(m, 128, stride=8), :], precision=HIGHEST, preferred_element_type=F32
        )
    sel[0:64, 0:128] = blocks
    spread = jnp.where(iota((128, COLS), 0) == place_of, 1.0, 0.0)
    wide = jnp.dot(sel[0:64, 0:128], spread, precision=HIGHEST, preferred_element_type=F32)
    sel[0:64, :] = wide
    at16 = iota((16, COLS), 0)
    old_cols = [
        jnp.sum(jnp.where(at16 == block_of, sel[m * 16 : (m + 1) * 16, :], 0.0), axis=0, keepdims=True)
        for m in range(M)
    ]
    for m in range(M):
        by_col[m : m + 1, :] = old_cols[m]

    arrive(grad_copies)
    for m in range(M):
        own[m].wait()
    arrive(row_copies)
    tile_sum = s_out[0, :, 256:384]
    for t in range(1, 8):
        tile_sum = tile_sum + s_out[t, :, 256:384]
    lane4 = iota((M, 128), 1)
    row_sum = jnp.sum(jnp.where(lane4 < ROWS, tile_sum, 0.0), axis=1, keepdims=True)
    weight_sum = jnp.sum(jnp.where(lane4 == ROWS, tile_sum, 0.0), axis=1, keepdims=True)
    two_y[y] = jnp.where(lane4 == 0, row_sum, jnp.where(lane4 == 1, weight_sum, 0.0))
    own_row = z * 4 + y
    for t in range(8):
        rows_out[own_row, t] = s_out[t, :, 256:384]
    sel[:, 128:256] = jnp.ones((128, 128), F32)
    for t in range(8):
        sel[t * 8 : t * 8 + M, 128:256] = s_out[t, :, 256:384]
    rnew[...] = 1.0 / jnp.transpose(sel[:, 128:256])[0:ROWS, :]

    for m in range(M):

        def add_columns(t, sums, m=m):
            plain, scaled = sums
            row = jnp.sum(jnp.where(lane32 == t * 8 + m, rnew[...], 0.0), axis=1, keepdims=True)
            g = g_in[t, m].astype(F32)
            sq = g * g
            by_rows = sq * row
            sq = sq + EPS
            for v in range(ROWS // 8):
                plain = plain + sq[v * 8 : (v + 1) * 8, :]
                scaled = scaled + by_rows[v * 8 : (v + 1) * 8, :]
            return plain, scaled

        nothing = jnp.zeros((8, COLS), F32)
        plain, scaled = lax.fori_loop(0, 8, add_columns, (nothing, nothing))
        red_y[y, m : m + 1, :] = jnp.sum(plain, axis=0, keepdims=True)
        red_y[y, M + m : M + m + 1, :] = jnp.sum(scaled, axis=0, keepdims=True)

    def reduce_over(axis, at, big, little, n):
        copies = []
        for d in LINE_PEERS:
            copies.append(to_line(axis, d, little.at[at], little.at[at], s_red.at[n + d - 1], r_red.at[n + d - 1]))
            copies.append(to_line(axis, d, big.at[at], big.at[at], s_red.at[n + d + 2], r_red.at[n + d + 2]))
        return begin(copies)

    stage = reduce_over("y", y, red_y, two_y, 0)
    own_rows = rows_out.at[pl.ds(own_row, 1)]
    rows_y = begin(
        [to_line("y", d, own_rows, own_rows, s_red.at[d + 11], r_red.at[d + 11]) for d in LINE_PEERS]
    )
    arrive(stage)
    sent += stage + rows_y
    red_z[z] = red_y[0] + red_y[1] + red_y[2] + red_y[3]
    two_z[z] = two_y[0] + two_y[1] + two_y[2] + two_y[3]
    stage = reduce_over("z", z, red_z, two_z, 6)
    arrive(rows_y)
    slab_rows = rows_out.at[pl.ds(pl.multiple_of(z * 4, 4), 4)]
    rows_z = begin(
        [to_line("z", d, slab_rows, slab_rows, s_red.at[d + 14], r_red.at[d + 14]) for d in LINE_PEERS]
    )
    arrive(stage)
    sent += stage + rows_z
    total = red_z[0] + red_z[1] + red_z[2] + red_z[3]
    two = two_z[0] + two_z[1] + two_z[2] + two_z[3]

    row_mean = two[:, 0:1] / D
    param_scale = jnp.sqrt(two[:, 1:2] / (D * FF) + 1e-6)
    col_new = DECAY * by_col[0:M, :] + (1.0 - DECAY) * total[0:M, :] / D
    sel[0:M, :] = col_new
    piece = lax.min(y * PIECE, COLS // 128 - PIECE)
    cols_out[y, k, :, 0 : PIECE * 128] = sel[0:M, pl.ds(pl.multiple_of(piece * 128, 128), PIECE * 128)]
    inv_col = 1.0 / col_new

    update_sum = jnp.sum(total[M : 2 * M, :] * inv_col, axis=1, keepdims=True) * row_mean
    cols_out[y, k, :, PIECE * 128 :] = jnp.broadcast_to(jnp.sum(update_sum, axis=0, keepdims=True), (M, 128))
    own_col = cols_out.at[y, k]
    cols_x = begin([to_cols(i, own_col, own_col, s_col.at[i], r_col.at[i]) for i in range(7)])
    sent += cols_x

    for n in range(FIRST, len(PARTS)):
        par_copies.append(send_params(n))

    arrive(cols_x)
    update_sum = cols_out[y, 0, 0:1, PIECE * 128 :]
    for t in range(1, 8):
        update_sum = update_sum + cols_out[y, t, 0:1, PIECE * 128 :]
    own_cols = cols_out.at[pl.ds(y, 1)]
    cols_y = begin(
        [to_line("y", d, own_cols, own_cols, s_col.at[d + 6], r_col.at[d + 6]) for d in LINE_PEERS]
    )
    sent += cols_y
    update_total = update_sum[0:1, 0:1]
    clip = jnp.maximum(1.0, jnp.sqrt(update_total / (M * D * FF)))
    factors = -(RATE * param_scale) / clip * jnp.sqrt(row_mean)
    factor = jnp.zeros((1, 128), F32)
    for m in range(M):
        own_factor = factors[m : m + 1, :]
        factor = factor + jnp.where(lax.rem(iota((1, 128), 1), 8) == m, own_factor, 0.0)
    by_row[...] = factor * jnp.sqrt(rnew[...])
    by_col[0:M, :] = jnp.sqrt(inv_col)

    def block_of_rows(t):
        return pl.ds(pl.multiple_of(t * ROWS, ROWS), ROWS)

    for m in range(M):
        col = by_col[m : m + 1, :]

        def put_change(t, carry, m=m, col=col):
            row = jnp.sum(jnp.where(lane32 == t * 8 + m, by_row[...], 0.0), axis=1, keepdims=True)
            change_out[m, block_of_rows(t), :] = (g_in[t, m].astype(F32) * row) * col
            return carry

        lax.fori_loop(0, 8, put_change, 0)
    arrive(rows_z)
    arrive(cols_y)
    for m in range(M):
        for n, part in enumerate(PARTS):
            if part[0] == m:
                arrive(par_copies[n])
        own[M + m].wait()
        if m == M - 1:
            break

        def put_weights(t, carry, m=m):
            new_out[m, block_of_rows(t), :] = decoded(p_out, s_out, t, m) + change_out[m, block_of_rows(t), :]
            return carry

        lax.fori_loop(0, 8, put_weights, 0)
    for cp in sent:
        cp.wait_send()


def apply_kernel(
    new_ref, change_ref, p_ref, s_ref, rows_ref, cols_ref, map_hbm,
    new_hbm, change_hbm, row_hbm, col_hbm,
    last_buf, row_buf, col_buf, new_map, big_sem, last_sem, small_sem,
):
    fetch = pltpu.make_async_copy(map_hbm, new_map, small_sem.at[0])
    fetch.start()
    big = [pltpu.make_async_copy(change_ref.at[m], change_hbm.at[m], big_sem.at[0, m]) for m in range(M)]
    big += [pltpu.make_async_copy(new_ref.at[m], new_hbm.at[m], big_sem.at[1, m]) for m in range(M - 1)]
    for cp in big:
        cp.start()

    last = []
    for t in range(8):
        rows = pl.ds(t * ROWS, ROWS)
        last_buf[rows, :] = decoded(p_ref, s_ref, t, M - 1) + change_ref[M - 1, rows, :]
        last.append(pltpu.make_async_copy(last_buf.at[rows], new_hbm.at[M - 1, rows], last_sem.at[t]))
        last[-1].start()

    fetch.wait()
    f = lax.axis_index(AXES)
    for n in range(M):
        b = new_map[n, f]
        row_buf[n : n + 1, :] = rows_ref[b // 8, lax.rem(b, 8), n : n + 1, 0:32]
        start = lax.rem(b, 16) * 80
        first = start // 128
        pair = []
        for t in (first, lax.min(first + 1, COLS // 128 - 1)):
            piece = lax.min(t // PIECE, 3)
            at = t - lax.min(piece * PIECE, COLS // 128 - PIECE)
            pair.append(cols_ref[piece, b // 16, n : n + 1, pl.ds(pl.multiple_of(at * 128, 128), 128)])
        pair = jnp.broadcast_to(jnp.concatenate(pair, axis=1), (8, 256))
        take = jnp.where(iota((256, 128), 0) == start - first * 128 + iota((256, 128), 1), 1.0, 0.0)
        got = jnp.dot(pair, take, precision=HIGHEST, preferred_element_type=F32)
        col_buf[n : n + 1, :] = got[0:1, 0:80]
    small = [
        pltpu.make_async_copy(row_buf, row_hbm, small_sem.at[1]),
        pltpu.make_async_copy(col_buf, col_hbm, small_sem.at[2]),
    ]
    for cp in small:
        cp.start()

    for cp in big + last + small:
        cp.wait()


def shards(params, grads, row_state_old, col_state_old, old_map, new_map):
    vmem = pl.BlockSpec(memory_space=pltpu.VMEM)
    hbm = pl.BlockSpec(memory_space=pltpu.HBM)
    dma = pltpu.SemaphoreType.DMA
    given = (params, grads, row_state_old, col_state_old, old_map)
    held = [pltpu.with_memory_space_constraint(a, pltpu.HBM) for a in given]
    held_map = pltpu.with_memory_space_constraint(new_map, pltpu.HBM)
    moved = pl.pallas_call(
        exchange_kernel,
        out_shape=[
            pltpu.VMEM((M - 1, 256, COLS), F32),
            pltpu.VMEM((M, 256, COLS), F32),
            pltpu.VMEM((8, M, ROWS, COLS), jnp.int16),
            pltpu.VMEM((8, M, 384), F32),
            pltpu.VMEM((16, 8, M, 128), F32),
            pltpu.VMEM((4, 8, M, (PIECE + 1) * 128), F32),
        ],
        in_specs=[hbm] * 5,
        out_specs=[vmem] * 6,
        scratch_shapes=[
            pltpu.VMEM((8, M, ROWS, COLS), jnp.bfloat16),
            pltpu.VMEM((ROWS, 128), F32),
            pltpu.VMEM((8, COLS), F32),
            pltpu.VMEM((M, ROWS, FF), jnp.bfloat16),
            pltpu.VMEM((M, ROWS, FF), F32),
            pltpu.VMEM((8, M, ROWS, COLS), jnp.int16),
            pltpu.VMEM((8, M, 384), F32),
            pltpu.VMEM((M, 32), F32),
            pltpu.VMEM((M, 80), F32),
            pltpu.VMEM((M, 128), jnp.int32),
            pltpu.VMEM((1024, 128), F32),
            pltpu.VMEM((4, 8, COLS), F32),
            pltpu.VMEM((4, 8, COLS), F32),
            pltpu.VMEM((4, M, 128), F32),
            pltpu.VMEM((4, M, 128), F32),
            pltpu.VMEM((128, COLS), F32),
            pltpu.VMEM((ROWS, 128), F32),
            pltpu.SemaphoreType.REGULAR,
            pltpu.SemaphoreType.REGULAR,
            pltpu.SemaphoreType.REGULAR,
            dma((2 * M,)),
            dma((3,)),
            dma((2 * M,)),
            dma((7,)), dma((7,)),
            dma((6,)), dma((6,)),
            dma((2, 7)), dma((2, 7)),
            dma((len(PARTS), 7)), dma((len(PARTS), 7)),
            dma((7,)), dma((7,)),
            dma((18,)), dma((18,)),
            dma((10,)), dma((10,)),
        ],
        compiler_params=pltpu.CompilerParams(
            collective_id=0, has_side_effects=True, vmem_limit_bytes=28 << 20
        ),
        name="exchange",
    )(*held)
    return pl.pallas_call(
        apply_kernel,
        out_shape=[
            jax.ShapeDtypeStruct((M, 256, COLS), F32),
            jax.ShapeDtypeStruct((M, 256, COLS), F32),
            jax.ShapeDtypeStruct((M, 32), F32),
            jax.ShapeDtypeStruct((M, 80), F32),
        ],
        in_specs=[vmem] * 6 + [hbm],
        out_specs=[hbm] * 4,
        scratch_shapes=[
            pltpu.VMEM((256, COLS), F32),
            pltpu.VMEM((M, 32), F32),
            pltpu.VMEM((M, 80), F32),
            pltpu.SMEM((M, 128), jnp.int32),
            dma((2, M)),
            dma((8,)),
            dma((3,)),
        ],
        compiler_params=pltpu.CompilerParams(vmem_limit_bytes=28 << 20),
        name="apply",
    )(*(pltpu.with_memory_space_constraint(a, pltpu.VMEM) for a in moved), held_map)


def solution(mesh):
    torus = Mesh(mesh.devices.reshape(4, 4, 4, 2), AXES)
    over = ("z", "y", "x", "c")
    return jax.shard_map(
        shards,
        mesh=torus,
        in_specs=(P(None, over, None), P(None, over, None), P(None, over), P(None, over), P(), P()),
        out_specs=(
            P(None, ("z", "y"), ("x", "c")),
            P(None, ("z", "y"), ("x", "c")),
            P(None, over),
            P(None, over),
        ),
        check_vma=False,
    )
```

```python
import math

import jax
import jax.numpy as jnp
from jax import lax
from jax.experimental import pallas as pl
from jax.experimental.pallas import tpu as pltpu
from jax.sharding import Mesh
from jax.sharding import PartitionSpec as P

D = 4096
FF = 10240
STEP = 4
M = 4
ROWS = 32
COLS = 1280
AXES = ("z", "y", "x", "c")
MESH = pl.DeviceIdType.MESH
HIGHEST = lax.Precision.HIGHEST
DECAY = 1.0 - float(STEP) ** (-0.8)
RATE = min(0.01, 1.0 / math.sqrt(STEP))
EPS = 1e-30
F32 = jnp.float32
TOP = 32767.0
PIECE = 3
PARTS = [(0, 0, 32), (1, 0, 32), (2, 0, 16), (2, 16, 16), (3, 0, 16), (3, 16, 16)]
FIRST = 3
LEADER = 4

COL_PEERS = [(1, 0), (3, 0), (1, 1), (3, 1), (0, 1), (2, 0), (2, 1)]
NEAR = 5
ORDER = (0, 1, 5, 2, 3, 6, 4)
LINE_PEERS = [1, 2, 3]


def iota(shape, dim):
    return lax.broadcasted_iota(jnp.int32, shape, dim)


def decoded(codes, steps, t, m):
    step = jnp.concatenate([steps[t, m : m + 1, 0:256]] * (COLS // 256), axis=1)
    return codes[t, m].astype(jnp.int32).astype(F32) * step


def exchange_kernel(
    params, grads, row_hbm, col_hbm, map_hbm,
    new_out, change_out, p_out, s_out, rows_out, cols_out,
    g_in, by_row, by_col, gv, pv, qv, sv, row_old, col_old, old_map, stored, red_y, red_z, two_y, two_z, sel, rnew,
    far_sem, lead_sem, go_sem, load_sem, small_sem, own_sem,
    s_tile, r_tile, s_line, r_line, s_grad, r_grad, s_par, r_par,
    s_row, r_row, s_red, r_red, s_col, r_col,
):
    z, y, x, c = (lax.axis_index(a) for a in AXES)
    k = x * 2 + c
    f = (z * 4 + y) * 8 + k

    def col_peer(i):
        dx, dc = COL_PEERS[i]
        return lax.rem(x + dx, 4), lax.rem(c + dc, 2)

    def to_cols(i, src, dst, ss, rs):
        tx, tc = col_peer(i)
        return pltpu.make_async_remote_copy(
            src_ref=src, dst_ref=dst, send_sem=ss, recv_sem=rs,
            device_id={"x": tx, "c": tc}, device_id_type=MESH,
        )

    def to_line(axis, d, src, dst, ss, rs):
        at = lax.rem((y if axis == "y" else z) + d, 4)
        return pltpu.make_async_remote_copy(
            src_ref=src, dst_ref=dst, send_sem=ss, recv_sem=rs,
            device_id={axis: at}, device_id_type=MESH,
        )

    def begin(copies):
        for cp in copies:
            cp.start()
        return copies

    def arrive(copies):
        for cp in copies:
            cp.wait_recv()

    barrier = pltpu.get_barrier_semaphore()
    for i in range(NEAR):
        tx, tc = col_peer(i)
        pl.semaphore_signal(barrier, inc=1, device_id={"x": tx, "c": tc}, device_id_type=MESH)

    def signal_lines(sem):
        for d in LINE_PEERS:
            pl.semaphore_signal(sem, inc=1, device_id={"y": lax.rem(y + d, 4)}, device_id_type=MESH)
            pl.semaphore_signal(sem, inc=1, device_id={"z": lax.rem(z + d, 4)}, device_id_type=MESH)

    @pl.when(k == LEADER)
    def _():
        signal_lines(barrier)


    small = [
        pltpu.make_async_copy(row_hbm, row_old, small_sem.at[0]),
        pltpu.make_async_copy(col_hbm, col_old, small_sem.at[1]),
        pltpu.make_async_copy(map_hbm, old_map, small_sem.at[2]),
    ]
    loads = []
    for m in range(M):
        loads.append(pltpu.make_async_copy(grads.at[m], gv.at[m], load_sem.at[m]))
    for m in range(M):
        loads.append(pltpu.make_async_copy(params.at[m], pv.at[m], load_sem.at[M + m]))
    begin(loads[0:1] + small + loads[1:])

    @pl.when(k == LEADER)
    def _():
        pl.semaphore_wait(barrier, NEAR + 6)

    @pl.when(k != LEADER)
    def _():
        pl.semaphore_wait(barrier, NEAR)


    def columns(i):
        tx, tc = col_peer(i)
        return pl.ds(pl.multiple_of((tx * 2 + tc) * COLS, 128), COLS)

    def send_grads(first, count, n, peers):
        part = pl.ds(first, count)
        copies = [
            to_cols(i, gv.at[part, :, columns(i)], g_in.at[k, part], s_grad.at[n, i], r_grad.at[n, i])
            for i in peers
        ]
        return begin(copies)

    pl.semaphore_signal(far_sem, inc=1, device_id={"x": lax.rem(x + 3, 4)}, device_id_type=MESH)
    loads[0].wait()
    grad_copies = send_grads(0, 1, 0, range(NEAR))
    pl.semaphore_wait(far_sem, 1)
    grad_copies += send_grads(0, 1, 0, range(NEAR, 7))

    @pl.when(k == LEADER)
    def _():
        signal_lines(lead_sem)

    mine = stored.at[pl.ds(pl.multiple_of(f * 8, 8), 8)]
    mine[...] = jnp.zeros((8, 128), F32)
    for cp in small:
        cp.wait()
    mine[0:4, 0:80] = col_old[...]
    mine[4:8, 0:32] = row_old[...]

    tiles = begin([to_cols(i, mine, mine, s_tile.at[i], r_tile.at[i]) for i in range(7)])
    for m in range(1, M):
        loads[m].wait()
    grad_copies += send_grads(1, M - 1, 1, ORDER)
    sent = tiles + grad_copies

    def peer_block(i):
        tx, tc = col_peer(i)
        return tx * 2 + tc

    def send_params(n):
        m, first, count = PARTS[n]
        rows = pl.ds(first, count)
        copies = begin(
            [
                to_cols(i, qv.at[peer_block(i), m, rows], p_out.at[k, m, rows], s_par.at[n, i], r_par.at[n, i])
                for i in ORDER
            ]
        )
        sent.extend(copies)
        return copies

    par_copies = []
    own_columns = pl.ds(pl.multiple_of(k * COLS, 128), COLS)
    lane32 = iota((ROWS, 128), 1)
    row_sums = jnp.zeros((ROWS, 128), F32)
    own = []
    for m in range(M):

        def add_squares(t, acc, m=m):
            g = gv[m, :, pl.ds(pl.multiple_of(t * COLS, 128), COLS)].astype(F32)
            sq = g * g + EPS
            for u in range(COLS // 128):
                acc = acc + sq[:, u * 128 : (u + 1) * 128]
            return acc

        part = lax.fori_loop(0, 8, add_squares, jnp.zeros((ROWS, 128), F32))
        total = jnp.sum(part, axis=1, keepdims=True)
        row_sums = row_sums + jnp.where(lane32 == m, total, 0.0)
        own.append(pltpu.make_async_copy(gv.at[m, :, own_columns], g_in.at[k, m], own_sem.at[m]))
        own[-1].start()

    at8 = iota((8, 128), 0)
    lane8 = iota((8, 128), 1)
    squares = jnp.zeros((8, 128), F32)
    for m in range(M):
        loads[M + m].wait()

        def add_weights(t, acc, m=m):
            w = pv[m, :, pl.ds(pl.multiple_of(t * COLS, 128), COLS)]
            sq = w * w
            tops = [jnp.zeros((8, 128), F32)] * 2
            size = jnp.abs(w)
            for u in range(COLS // 128):
                for v in range(ROWS // 8):
                    acc = acc + sq[v * 8 : (v + 1) * 8, u * 128 : (u + 1) * 128]
                    tops[u % 2] = jnp.maximum(tops[u % 2], size[v * 8 : (v + 1) * 8, u * 128 : (u + 1) * 128])
            top = jnp.concatenate([jnp.max(a, axis=0, keepdims=True) for a in tops], axis=1)
            top = jnp.maximum(top, 1e-30)
            sv[t, m : m + 1, 0:256] = top * (1.0 / TOP)
            per = jnp.concatenate([TOP / top] * (COLS // 256), axis=1)
            qv[t, m] = jnp.round(w * per).astype(jnp.int32).astype(jnp.int16)
            return acc

        part = lax.fori_loop(0, 8, add_weights, jnp.zeros((8, 128), F32))
        total = jnp.sum(jnp.sum(part, axis=1, keepdims=True), axis=0, keepdims=True)
        squares = squares + jnp.where((at8 == m) & (lane8 == ROWS), total, 0.0)
        own.append(pltpu.make_async_copy(qv.at[k, m], p_out.at[k, m], own_sem.at[M + m]))
        own[-1].start()

    arrive(tiles)

    @pl.when(k == LEADER)
    def _():
        pl.semaphore_wait(lead_sem, 6)
        for i in range(7):
            tx, tc = col_peer(i)
            pl.semaphore_signal(go_sem, inc=1, device_id={"x": tx, "c": tc}, device_id_type=MESH)

    @pl.when(k != LEADER)
    def _():
        pl.semaphore_wait(go_sem, 1)

    line_at = stored.at[pl.ds(pl.multiple_of((z * 4 + y) * 64, 64), 64)]
    lines = begin([to_line("y", d, line_at, line_at, s_line.at[d - 1], r_line.at[d - 1]) for d in LINE_PEERS])
    sent += lines

    arrive(lines)
    slab_at = stored.at[pl.ds(pl.multiple_of(z * 256, 256), 256)]
    slabs = begin([to_line("z", d, slab_at, slab_at, s_line.at[d + 2], r_line.at[d + 2]) for d in LINE_PEERS])
    sent += slabs
    arrive(slabs)

    at_row = iota((128, 128), 0)
    picked = jnp.zeros((128, 128), F32)
    for m in range(M):
        onehot = jnp.where((at_row == m) & (old_map[m : m + 1, :] == f), 1.0, 0.0)
        picked = picked + jnp.dot(
            onehot, stored[pl.ds(4 + m, 128, stride=8), :], precision=HIGHEST, preferred_element_type=F32
        )
    sel[...] = jnp.zeros((128, COLS), F32)
    sel[0:ROWS, 0:128] = row_sums
    row_sums = jnp.transpose(sel[:, 0:128])[0:8, :]
    row_new = DECAY * picked[0:8, :] + (1.0 - DECAY) * row_sums / FF
    row_new = jnp.where((at8 < M) & (lane8 < ROWS), row_new, 1.0)
    own_tile = jnp.where(lane8 == ROWS, squares, row_new)[0:M, :]
    for t in range(8):
        sv[t, :, 256:384] = own_tile
    s_out[k] = sv[k]
    row_copies = begin([to_cols(i, sv.at[peer_block(i)], s_out.at[k], s_row.at[i], r_row.at[i]) for i in range(7)])
    sent += row_copies
    for n in range(FIRST):
        par_copies.append(send_params(n))

    lane = iota((1, COLS), 1)
    block_of = ((lane.astype(F32) + 0.5) * (1.0 / 80.0)).astype(jnp.int32)
    place_of = lane - 80 * block_of
    at64 = iota((64, 128), 0)
    blocks = jnp.zeros((64, 128), F32)
    for m in range(M):
        wanted = (at64 - 16 * m) + k * 16
        inside = (at64 >= 16 * m) & (at64 < 16 * m + 16)
        onehot = jnp.where(inside & (old_map[m : m + 1, :] == wanted), 1.0, 0.0)
        blocks = blocks + jnp.dot(
            onehot, stored[pl.ds(m, 128, stride=8), :], precision=HIGHEST, preferred_element_type=F32
        )
    sel[0:64, 0:128] = blocks
    spread = jnp.where(iota((128, COLS), 0) == place_of, 1.0, 0.0)
    wide = jnp.dot(sel[0:64, 0:128], spread, precision=HIGHEST, preferred_element_type=F32)
    sel[0:64, :] = wide
    at16 = iota((16, COLS), 0)
    old_cols = [
        jnp.sum(jnp.where(at16 == block_of, sel[m * 16 : (m + 1) * 16, :], 0.0), axis=0, keepdims=True)
        for m in range(M)
    ]
    for m in range(M):
        by_col[m : m + 1, :] = old_cols[m]

    arrive(grad_copies)
    for m in range(M):
        own[m].wait()
    arrive(row_copies)
    tile_sum = s_out[0, :, 256:384]
    for t in range(1, 8):
        tile_sum = tile_sum + s_out[t, :, 256:384]
    lane4 = iota((M, 128), 1)
    row_sum = jnp.sum(jnp.where(lane4 < ROWS, tile_sum, 0.0), axis=1, keepdims=True)
    weight_sum = jnp.sum(jnp.where(lane4 == ROWS, tile_sum, 0.0), axis=1, keepdims=True)
    two_y[y] = jnp.where(lane4 == 0, row_sum, jnp.where(lane4 == 1, weight_sum, 0.0))
    own_row = z * 4 + y
    for t in range(8):
        rows_out[own_row, t] = s_out[t, :, 256:384]
    sel[:, 128:256] = jnp.ones((128, 128), F32)
    for t in range(8):
        sel[t * 8 : t * 8 + M, 128:256] = s_out[t, :, 256:384]
    rnew[...] = 1.0 / jnp.transpose(sel[:, 128:256])[0:ROWS, :]

    for m in range(M):

        def add_columns(t, sums, m=m):
            plain, scaled = sums
            row = jnp.sum(jnp.where(lane32 == t * 8 + m, rnew[...], 0.0), axis=1, keepdims=True)
            g = g_in[t, m].astype(F32)
            sq = g * g
            by_rows = sq * row
            sq = sq + EPS
            for v in range(ROWS // 8):
                plain = plain + sq[v * 8 : (v + 1) * 8, :]
                scaled = scaled + by_rows[v * 8 : (v + 1) * 8, :]
            return plain, scaled

        nothing = jnp.zeros((8, COLS), F32)
        plain, scaled = lax.fori_loop(0, 8, add_columns, (nothing, nothing))
        red_y[y, m : m + 1, :] = jnp.sum(plain, axis=0, keepdims=True)
        red_y[y, M + m : M + m + 1, :] = jnp.sum(scaled, axis=0, keepdims=True)

    def reduce_over(axis, at, big, little, n):
        copies = []
        for d in LINE_PEERS:
            copies.append(to_line(axis, d, little.at[at], little.at[at], s_red.at[n + d - 1], r_red.at[n + d - 1]))
            copies.append(to_line(axis, d, big.at[at], big.at[at], s_red.at[n + d + 2], r_red.at[n + d + 2]))
        return begin(copies)

    stage = reduce_over("y", y, red_y, two_y, 0)
    own_rows = rows_out.at[pl.ds(own_row, 1)]
    rows_y = begin(
        [to_line("y", d, own_rows, own_rows, s_red.at[d + 11], r_red.at[d + 11]) for d in LINE_PEERS]
    )
    arrive(stage)
    sent += stage + rows_y
    red_z[z] = red_y[0] + red_y[1] + red_y[2] + red_y[3]
    two_z[z] = two_y[0] + two_y[1] + two_y[2] + two_y[3]
    stage = reduce_over("z", z, red_z, two_z, 6)
    arrive(rows_y)
    slab_rows = rows_out.at[pl.ds(pl.multiple_of(z * 4, 4), 4)]
    rows_z = begin(
        [to_line("z", d, slab_rows, slab_rows, s_red.at[d + 14], r_red.at[d + 14]) for d in LINE_PEERS]
    )
    arrive(stage)
    sent += stage + rows_z
    total = red_z[0] + red_z[1] + red_z[2] + red_z[3]
    two = two_z[0] + two_z[1] + two_z[2] + two_z[3]

    row_mean = two[:, 0:1] / D
    param_scale = jnp.sqrt(two[:, 1:2] / (D * FF) + 1e-6)
    col_new = DECAY * by_col[0:M, :] + (1.0 - DECAY) * total[0:M, :] / D
    sel[0:M, :] = col_new
    piece = lax.min(y * PIECE, COLS // 128 - PIECE)
    cols_out[y, k, :, 0 : PIECE * 128] = sel[0:M, pl.ds(pl.multiple_of(piece * 128, 128), PIECE * 128)]
    inv_col = 1.0 / col_new

    update_sum = jnp.sum(total[M : 2 * M, :] * inv_col, axis=1, keepdims=True) * row_mean
    cols_out[y, k, :, PIECE * 128 :] = jnp.broadcast_to(jnp.sum(update_sum, axis=0, keepdims=True), (M, 128))
    own_col = cols_out.at[y, k]
    cols_x = begin([to_cols(i, own_col, own_col, s_col.at[i], r_col.at[i]) for i in range(7)])
    sent += cols_x

    for n in range(FIRST, len(PARTS)):
        par_copies.append(send_params(n))

    arrive(cols_x)
    update_sum = cols_out[y, 0, 0:1, PIECE * 128 :]
    for t in range(1, 8):
        update_sum = update_sum + cols_out[y, t, 0:1, PIECE * 128 :]
    own_cols = cols_out.at[pl.ds(y, 1)]
    cols_y = begin(
        [to_line("y", d, own_cols, own_cols, s_col.at[d + 6], r_col.at[d + 6]) for d in LINE_PEERS]
    )
    sent += cols_y
    update_total = update_sum[0:1, 0:1]
    clip = jnp.maximum(1.0, jnp.sqrt(update_total / (M * D * FF)))
    factors = -(RATE * param_scale) / clip * jnp.sqrt(row_mean)
    factor = jnp.zeros((1, 128), F32)
    for m in range(M):
        own_factor = factors[m : m + 1, :]
        factor = factor + jnp.where(lax.rem(iota((1, 128), 1), 8) == m, own_factor, 0.0)
    by_row[...] = factor * jnp.sqrt(rnew[...])
    by_col[0:M, :] = jnp.sqrt(inv_col)

    def block_of_rows(t):
        return pl.ds(pl.multiple_of(t * ROWS, ROWS), ROWS)

    for m in range(M):
        col = by_col[m : m + 1, :]

        def put_change(t, carry, m=m, col=col):
            row = jnp.sum(jnp.where(lane32 == t * 8 + m, by_row[...], 0.0), axis=1, keepdims=True)
            change_out[m, block_of_rows(t), :] = (g_in[t, m].astype(F32) * row) * col
            return carry

        lax.fori_loop(0, 8, put_change, 0)
    arrive(rows_z)
    arrive(cols_y)
    for m in range(M):
        for n, part in enumerate(PARTS):
            if part[0] == m:
                arrive(par_copies[n])
        own[M + m].wait()
        if m == M - 1:
            break

        def put_weights(t, carry, m=m):
            new_out[m, block_of_rows(t), :] = decoded(p_out, s_out, t, m) + change_out[m, block_of_rows(t), :]
            return carry

        lax.fori_loop(0, 8, put_weights, 0)
    for cp in sent:
        cp.wait_send()


def apply_kernel(
    new_ref, change_ref, p_ref, s_ref, rows_ref, cols_ref, map_hbm,
    new_hbm, change_hbm, row_hbm, col_hbm,
    last_buf, row_buf, col_buf, new_map, big_sem, last_sem, small_sem,
):
    fetch = pltpu.make_async_copy(map_hbm, new_map, small_sem.at[0])
    fetch.start()
    big = [pltpu.make_async_copy(change_ref.at[m], change_hbm.at[m], big_sem.at[0, m]) for m in range(M)]
    big += [pltpu.make_async_copy(new_ref.at[m], new_hbm.at[m], big_sem.at[1, m]) for m in range(M - 1)]
    for cp in big:
        cp.start()

    last = []
    for t in range(8):
        rows = pl.ds(t * ROWS, ROWS)
        last_buf[rows, :] = decoded(p_ref, s_ref, t, M - 1) + change_ref[M - 1, rows, :]
        last.append(pltpu.make_async_copy(last_buf.at[rows], new_hbm.at[M - 1, rows], last_sem.at[t]))
        last[-1].start()

    fetch.wait()
    f = lax.axis_index(AXES)
    for n in range(M):
        b = new_map[n, f]
        row_buf[n : n + 1, :] = rows_ref[b // 8, lax.rem(b, 8), n : n + 1, 0:32]
        start = lax.rem(b, 16) * 80
        first = start // 128
        pair = []
        for t in (first, lax.min(first + 1, COLS // 128 - 1)):
            piece = lax.min(t // PIECE, 3)
            at = t - lax.min(piece * PIECE, COLS // 128 - PIECE)
            pair.append(cols_ref[piece, b // 16, n : n + 1, pl.ds(pl.multiple_of(at * 128, 128), 128)])
        pair = jnp.broadcast_to(jnp.concatenate(pair, axis=1), (8, 256))
        take = jnp.where(iota((256, 128), 0) == start - first * 128 + iota((256, 128), 1), 1.0, 0.0)
        got = jnp.dot(pair, take, precision=HIGHEST, preferred_element_type=F32)
        col_buf[n : n + 1, :] = got[0:1, 0:80]
    small = [
        pltpu.make_async_copy(row_buf, row_hbm, small_sem.at[1]),
        pltpu.make_async_copy(col_buf, col_hbm, small_sem.at[2]),
    ]
    for cp in small:
        cp.start()

    for cp in big + last + small:
        cp.wait()


def shards(params, grads, row_state_old, col_state_old, old_map, new_map):
    vmem = pl.BlockSpec(memory_space=pltpu.VMEM)
    hbm = pl.BlockSpec(memory_space=pltpu.HBM)
    dma = pltpu.SemaphoreType.DMA
    given = (params, grads, row_state_old, col_state_old, old_map)
    held = [pltpu.with_memory_space_constraint(a, pltpu.HBM) for a in given]
    held_map = pltpu.with_memory_space_constraint(new_map, pltpu.HBM)
    moved = pl.pallas_call(
        exchange_kernel,
        out_shape=[
            pltpu.VMEM((M - 1, 256, COLS), F32),
            pltpu.VMEM((M, 256, COLS), F32),
            pltpu.VMEM((8, M, ROWS, COLS), jnp.int16),
            pltpu.VMEM((8, M, 384), F32),
            pltpu.VMEM((16, 8, M, 128), F32),
            pltpu.VMEM((4, 8, M, (PIECE + 1) * 128), F32),
        ],
        in_specs=[hbm] * 5,
        out_specs=[vmem] * 6,
        scratch_shapes=[
            pltpu.VMEM((8, M, ROWS, COLS), jnp.bfloat16),
            pltpu.VMEM((ROWS, 128), F32),
            pltpu.VMEM((8, COLS), F32),
            pltpu.VMEM((M, ROWS, FF), jnp.bfloat16),
            pltpu.VMEM((M, ROWS, FF), F32),
            pltpu.VMEM((8, M, ROWS, COLS), jnp.int16),
            pltpu.VMEM((8, M, 384), F32),
            pltpu.VMEM((M, 32), F32),
            pltpu.VMEM((M, 80), F32),
            pltpu.VMEM((M, 128), jnp.int32),
            pltpu.VMEM((1024, 128), F32),
            pltpu.VMEM((4, 8, COLS), F32),
            pltpu.VMEM((4, 8, COLS), F32),
            pltpu.VMEM((4, M, 128), F32),
            pltpu.VMEM((4, M, 128), F32),
            pltpu.VMEM((128, COLS), F32),
            pltpu.VMEM((ROWS, 128), F32),
            pltpu.SemaphoreType.REGULAR,
            pltpu.SemaphoreType.REGULAR,
            pltpu.SemaphoreType.REGULAR,
            dma((2 * M,)),
            dma((3,)),
            dma((2 * M,)),
            dma((7,)), dma((7,)),
            dma((6,)), dma((6,)),
            dma((2, 7)), dma((2, 7)),
            dma((len(PARTS), 7)), dma((len(PARTS), 7)),
            dma((7,)), dma((7,)),
            dma((18,)), dma((18,)),
            dma((10,)), dma((10,)),
        ],
        compiler_params=pltpu.CompilerParams(
            collective_id=0, has_side_effects=True, vmem_limit_bytes=28 << 20
        ),
        name="exchange",
    )(*held)
    return pl.pallas_call(
        apply_kernel,
        out_shape=[
            jax.ShapeDtypeStruct((M, 256, COLS), F32),
            jax.ShapeDtypeStruct((M, 256, COLS), F32),
            jax.ShapeDtypeStruct((M, 32), F32),
            jax.ShapeDtypeStruct((M, 80), F32),
        ],
        in_specs=[vmem] * 6 + [hbm],
        out_specs=[hbm] * 4,
        scratch_shapes=[
            pltpu.VMEM((256, COLS), F32),
            pltpu.VMEM((M, 32), F32),
            pltpu.VMEM((M, 80), F32),
            pltpu.SMEM((M, 128), jnp.int32),
            dma((2, M)),
            dma((8,)),
            dma((3,)),
        ],
        compiler_params=pltpu.CompilerParams(vmem_limit_bytes=28 << 20),
        name="apply",
    )(*(pltpu.with_memory_space_constraint(a, pltpu.VMEM) for a in moved), held_map)


def solution(mesh):
    torus = Mesh(mesh.devices.reshape(4, 4, 4, 2), AXES)
    over = ("z", "y", "x", "c")
    return jax.shard_map(
        shards,
        mesh=torus,
        in_specs=(P(None, over, None), P(None, over, None), P(None, over), P(None, over), P(), P()),
        out_specs=(
            P(None, ("z", "y"), ("x", "c")),
            P(None, ("z", "y"), ("x", "c")),
            P(None, over),
            P(None, over),
        ),
        check_vma=False,
    )
```
